256 devices in a mesh: gx: 4 (over y), gy: 8 (over x, core), gz: 8 (over z).
Axes of the slice: x: 4, y: 4, z: 8, core: 2. Of those that a mesh axis runs over, the one named last changes fastest.
Arguments:
- positions: float32 [3, 32768, 128], P(None, ('gx', 'gy', 'gz')), may hold values from 0 to 1, as said below
- charges: float32 [32768, 128], P(('gx', 'gy', 'gz')), may hold values from -6 to 6
- velocities: float32 [3, 32768, 128], P(None, ('gx', 'gy', 'gz')), may hold values from -6 to 6
- leaf_ids: int32 [32768], P(('gx', 'gy', 'gz')), may hold values from 0 to 2097151, as said below
- live_counts: int32 [256], replicated, may hold values from 32 to 96
- send_counts: int32 [8, 256], replicated, may hold values from 0 to 32, as said below
Outputs:
- moved_positions: float32 [3, 32768, 128], P(None, ('gx', 'gy', 'gz'))
- moved_charges: float32 [32768, 128], P(('gx', 'gy', 'gz'))
- moved_velocities: float32 [3, 32768, 128], P(None, ('gx', 'gy', 'gz'))
- moved_leaves: int32 [32768], P(('gx', 'gy', 'gz'))
- leaf_moments: float32 [286, 32768], P(None, ('gx', 'gy', 'gz'))
- parent_moments: float32 [286, 32768], P(None, ('gx', 'gy', 'gz'))
The draws below stay inside these ranges and needn't reach their ends.
Inputs may be any that keep to these rules, and one draw needn't show every extreme that they name: `positions`: every particle of a live slot lies inside the leaf cell of side 2^-7 named by the slot's leaf index. `leaf_ids`: morton indices of cells at depth 7; a leaf's parent cell is its index // 8. `send_counts`: no device sends more blocks than it holds live; after every section no device holds more than 128 live blocks; in every draw some device sends exactly 32 blocks in the first section and its partner then holds exactly 128.
All inputs are finite; a program needn't handle non-finite values.
Results may differ from the reference program's by a relative error of at most 0.0003.
Values sent between devices are 32-bit elements; how exact they have to be, the bound alone decides.
A program may use at most 128 MiB of HBM per device.

```python
import math
from functools import partial
import jax
import jax.numpy as jnp
import numpy as np
from jax import lax

CAP = 128
PART = 128
ORDER = 10
LEVEL = 7
SEND_CAP = 32
SECTIONS = 8
NCOEF = 286
BLOCKS = 32768
N_GX = 4
N_GY = 8
DEVICES = 256


def leaf_table(key):
    base_key = jax.random.fold_in(key, 11)
    climb_key, start_key, octant_key, order_key = jax.random.split(base_key, 4)
    climbs = (jax.random.randint(climb_key, (DEVICES, CAP), 0, 3) == 0).astype(jnp.int32)
    parents = jax.random.randint(start_key, (DEVICES, 1), 0, 8 ** (LEVEL - 1) - CAP) + jnp.cumsum(climbs, axis=1)
    row_keys = jax.random.split(order_key, DEVICES)
    parents = jax.vmap(jax.random.permutation)(row_keys, parents)
    octants = jax.random.randint(octant_key, (DEVICES, CAP), 0, 8)
    return (parents * 8 + octants).reshape(DEVICES * CAP).astype(jnp.int32)


def route_plan(key):
    base_key = jax.random.fold_in(key, 37)
    start_key, pair_key, section_key = jax.random.split(base_key, 3)
    quarter = CAP // 4
    live_now = jax.random.randint(start_key, (DEVICES,), quarter, 3 * quarter + 1)
    half_way = DEVICES // 2
    chosen = jax.random.randint(pair_key, (), 0, half_way)
    live_now = live_now.at[chosen].set(3 * quarter).at[chosen + half_way].set(3 * quarter)
    initial = live_now
    everyone = jnp.arange(DEVICES, dtype=jnp.int32)
    outer_bits = int(N_GX).bit_length() - 1
    middle_bits = int(N_GY).bit_length() - 1
    phase_firsts = [0, outer_bits, outer_bits + middle_bits]
    sender = chosen.astype(jnp.int32)
    holder = (chosen + half_way).astype(jnp.int32)
    count_rows = []
    for section_num in range(SECTIONS):
        bit_mask = 1 << SECTIONS - 1 - section_num
        partner = jnp.bitwise_xor(everyone, bit_mask)
        lower_half = jnp.bitwise_and(everyone, bit_mask) == 0
        phase_start = section_num in phase_firsts
        if phase_start and section_num > 0:
            sender = jnp.argmax(live_now).astype(jnp.int32)
            holder = jnp.bitwise_xor(sender, bit_mask)
        is_sender = everyone == sender
        is_holder = everyone == holder
        low_key, high_key = jax.random.split(jax.random.fold_in(section_key, section_num))
        low_count = jax.random.randint(low_key, (DEVICES,), 0, jnp.minimum(live_now, SEND_CAP) + 1)
        if phase_start:
            low_count = jnp.where(is_sender, SEND_CAP, low_count)
            low_count = jnp.where(is_holder, jnp.maximum(low_count, live_now + SEND_CAP - CAP), low_count)
        else:
            spare_room = CAP - live_now[holder]
            low_count = jnp.where(is_holder, 0, low_count)
            low_count = jnp.where(partner == holder, jnp.minimum(low_count, spare_room), low_count)
        paired_count = low_count[partner]
        held_count = live_now[partner]
        lowest = jnp.maximum(0, live_now + paired_count - CAP)
        highest = jnp.maximum(lowest, jnp.minimum(jnp.minimum(live_now, SEND_CAP), CAP - held_count + paired_count))
        high_count = jax.random.randint(high_key, (DEVICES,), lowest, highest + 1)
        if phase_start:
            high_count = jnp.where(is_sender, SEND_CAP, high_count)
        else:
            high_count = jnp.where(is_holder, 0, high_count)
        if section_num == 0:
            high_count = jnp.where(is_holder, 0, high_count)
        counts = jnp.where(lower_half, low_count, high_count)
        count_rows.append(counts)
        live_now = live_now - counts + counts[partner]
    return (initial.astype(jnp.int32), jnp.stack(count_rows).astype(jnp.int32))


def draw_leaf_ids(key, part):
    return leaf_table(key)


def draw_live_counts(key, part):
    return route_plan(key)[0]


def draw_send_counts(key, part):
    return route_plan(key)[1]


def draw_positions(key, part):
    leaves = leaf_table(key)
    coordinates = []
    for axis_bit in (2, 1, 0):
        coordinate = jnp.zeros_like(leaves)
        for level_num in range(LEVEL):
            octant_id = jnp.right_shift(leaves, 3 * level_num)
            coordinate = coordinate + jnp.left_shift(jnp.bitwise_and(jnp.right_shift(octant_id, axis_bit), 1), level_num)
        coordinates.append(coordinate.astype(jnp.float32))
    cell_grid = jnp.stack(coordinates)
    fraction = jax.random.uniform(jax.random.fold_in(key, 23), (3, DEVICES * CAP, PART), jnp.float32, 0.0, 1.0)
    fraction = 0.001 + 0.998 * fraction
    return ((cell_grid[:, :, None] + fraction) / float(2 ** LEVEL)).astype(jnp.float32)


def level_of(own_key, dims, cuts, low, largest):
    loudness, own = 1.0, jax.random.fold_in(own_key, 6)
    for axis_at, blocks in cuts:
        heights = jnp.exp(jax.random.uniform(jax.random.fold_in(own, axis_at), (blocks,), jnp.float32, low / len(cuts), largest / len(cuts)))
        loudness = loudness * jnp.repeat(heights, dims[axis_at] // blocks).reshape([-1 if axis == axis_at else 1 for axis in range(len(dims))])
    return loudness


def noise(own_key, shape, deviation, bound, cuts=(), kind=jnp.bfloat16):
    factor_of = level_of(own_key, shape, cuts, -0.22, 0.18) if cuts else 1.0
    entries = jax.random.normal(own_key, shape, jnp.float32) * deviation * factor_of
    return jnp.minimum(jnp.maximum(entries, -bound), bound).astype(kind)


def setup_inputs(seed: int = 0) -> dict:
    streams_of = jax.random.split(jax.random.key(seed), 7)
    positions = draw_positions(jax.random.fold_in(streams_of[6], 71), 0)
    charges = noise(streams_of[1], (BLOCKS, PART), 1.0, 6.0, ((0, 256),), jnp.float32)
    velocities = noise(streams_of[2], (3, BLOCKS, PART), 1.0, 6.0, ((1, 256),), jnp.float32)
    leaf_ids = draw_leaf_ids(jax.random.fold_in(streams_of[6], 71), 0)
    live_counts = draw_live_counts(jax.random.fold_in(streams_of[6], 71), 0)
    send_counts = draw_send_counts(jax.random.fold_in(streams_of[6], 71), 0)
    return dict(positions=positions, charges=charges, velocities=velocities, leaf_ids=leaf_ids, live_counts=live_counts, send_counts=send_counts)


def exponents(max_order):
    return [(p, q, r) for p in range(max_order + 1) for q in range(max_order + 1 - p) for r in range(max_order + 1 - p - q)]


def shift_tables(max_order):
    triples = exponents(max_order)
    count = len(triples)
    tables = np.zeros((8, count, count))
    for octant_id in range(8):
        signs = [0.5 if (octant_id >> shift_bit) & 1 else -0.5 for shift_bit in (2, 1, 0)]
        for k, (p, q, r) in enumerate(triples):
            for j, (e, f, g) in enumerate(triples):
                if e <= p and f <= q and g <= r:
                    tables[octant_id, k, j] = (math.comb(p, e) * math.comb(q, f) * math.comb(r, g)
                                               * signs[0] ** (p - e) * signs[1] ** (q - f) * signs[2] ** (r - g)
                                               * 0.5 ** (e + f + g))
    return jnp.asarray(tables, jnp.float32)


def morton_cells(leaves, tree_depth):
    coordinates = []
    for axis_bit in (2, 1, 0):
        coordinate = jnp.zeros_like(leaves)
        for level_num in range(tree_depth):
            octant_id = jnp.right_shift(leaves, 3 * level_num)
            coordinate = coordinate + jnp.left_shift(jnp.bitwise_and(jnp.right_shift(octant_id, axis_bit), 1), level_num)
        coordinates.append(coordinate)
    return coordinates


def leaf_moments(positions, charges, leaves, max_order, tree_depth):
    cells_side = float(2 ** tree_depth)
    coordinates = morton_cells(leaves, tree_depth)
    powers = []
    for axis_num in range(3):
        offset_row = 2.0 * (positions[axis_num] * cells_side - coordinates[axis_num].astype(jnp.float32)[:, None]) - 1.0
        power_list = [jnp.ones_like(offset_row)]
        for degree_num in range(max_order):
            power_list.append(power_list[-1] * offset_row)
        powers.append(power_list)
    exponent_pairs = [(p, q) for p in range(max_order + 1) for q in range(max_order + 1 - p)]
    weighted = jnp.stack([charges * powers[0][p] * powers[1][q] for p, q in exponent_pairs])
    third_powers = jnp.stack(powers[2])
    raw_sums = jnp.einsum('pbi,cbi->pcb', weighted, third_powers, precision=lax.Precision.HIGHEST)
    pieces = [raw_sums[n, :max_order + 1 - p - q] for n, (p, q) in enumerate(exponent_pairs)]
    return jnp.concatenate(pieces, axis=0) / 16.0


def parent_moments(moments, leaves, live_mask, tables):
    shifted = jnp.einsum('okj,jb->okb', tables, moments, precision=lax.Precision.HIGHEST)
    octant_id = jnp.bitwise_and(leaves, 7)
    chooser = (octant_id[None, :] == jnp.arange(8, dtype=jnp.int32)[:, None]).astype(jnp.float32)
    moved = jnp.sum(shifted * chooser[:, None, :], axis=0)
    parents = jnp.right_shift(leaves, 3)
    sibling = ((parents[:, None] == parents[None, :]) & live_mask[:, None] & live_mask[None, :]).astype(jnp.float32)
    return jnp.dot(moved, sibling, precision=lax.Precision.HIGHEST, preferred_element_type=jnp.float32)


def outgoing(blocks_now, live_count, sent_count, upper_half, slab_rows):
    start_at = jnp.where(upper_half, 0, live_count - sent_count).astype(jnp.int32)

    def cut(member):
        padding = jnp.zeros(member.shape[:1] + (slab_rows,) + member.shape[2:], member.dtype)
        return lax.dynamic_slice_in_dim(jnp.concatenate([member, padding], axis=1), start_at, slab_rows, 1)

    return jax.tree.map(cut, blocks_now)


def incoming(blocks_now, arrived, live_count, sent_count, got_count, upper_half):
    kept_count = live_count - sent_count

    def place(member, slab_part):
        slot_total = member.shape[1]
        slab_rows = slab_part.shape[1]
        edge_pad = jnp.zeros(member.shape[:1] + (slab_rows,) + member.shape[2:], member.dtype)
        wide_pad = jnp.zeros(member.shape, member.dtype)
        offset_old = jnp.where(upper_half, sent_count - got_count, 0)
        shifted = lax.dynamic_slice_in_dim(jnp.concatenate([edge_pad, member, edge_pad], axis=1),
                                           (slab_rows + offset_old).astype(jnp.int32), slot_total, 1)
        offset_new = jnp.where(upper_half, 0, kept_count)
        placed = lax.dynamic_slice_in_dim(jnp.concatenate([wide_pad, slab_part, wide_pad], axis=1),
                                          (slot_total - offset_new).astype(jnp.int32), slot_total, 1)
        slot_ids = jnp.arange(slot_total, dtype=jnp.int32)
        take_new = jnp.where(upper_half, slot_ids < got_count, (slot_ids >= kept_count) & (slot_ids < kept_count + got_count))
        take_old = jnp.where(upper_half, (slot_ids >= got_count) & (slot_ids < got_count + kept_count), slot_ids < kept_count)
        shape_mask = (1, slot_total) + (1,) * (member.ndim - 2)
        take_new = take_new.reshape(shape_mask)
        take_old = take_old.reshape(shape_mask)
        return jnp.where(take_new, placed, jnp.where(take_old, shifted, jnp.zeros_like(member)))

    return jax.tree.map(place, blocks_now, arrived)


def reference(positions, charges, velocities, leaf_ids, live_counts, send_counts):
    blocks_now = (jnp.moveaxis(positions.reshape(3, DEVICES, CAP, PART), 1, 0),
                  charges.reshape(DEVICES, 1, CAP, PART),
                  jnp.moveaxis(velocities.reshape(3, DEVICES, CAP, PART), 1, 0),
                  leaf_ids.astype(jnp.float32).reshape(DEVICES, 1, CAP))
    everyone = jnp.arange(DEVICES, dtype=jnp.int32)
    live_all = live_counts
    send_out = partial(outgoing, slab_rows=SEND_CAP)
    for section_num in range(SECTIONS):
        bit_mask = 1 << (SECTIONS - 1 - section_num)
        partner = jnp.bitwise_xor(everyone, bit_mask)
        upper_half = jnp.bitwise_and(everyone, bit_mask) != 0
        sent_count = send_counts[section_num]
        got_count = sent_count[partner]
        outbound = jax.vmap(send_out)(blocks_now, live_all, sent_count, upper_half)
        arrived = jax.tree.map(lambda member: member[partner], outbound)
        blocks_now = jax.vmap(incoming)(blocks_now, arrived, live_all, sent_count, got_count, upper_half)
        live_all = live_all - sent_count + got_count
    tables = shift_tables(ORDER)

    def settle(inputs):
        device_positions, device_charges, device_leaves, live_count = inputs
        live_mask = jnp.arange(CAP, dtype=jnp.int32) < live_count
        leaves = jnp.where(live_mask, device_leaves[0].astype(jnp.int32), 0)
        leaf_part = leaf_moments(device_positions, device_charges[0], leaves, ORDER, LEVEL)
        return leaf_part, parent_moments(leaf_part, leaves, live_mask, tables)

    leaf_part, parent_part = lax.map(settle, (blocks_now[0], blocks_now[1], blocks_now[3], live_all))
    all_mask = jnp.arange(CAP, dtype=jnp.int32)[None, :] < live_all[:, None]
    moved_leaves = jnp.where(all_mask, blocks_now[3][:, 0].astype(jnp.int32), -1).reshape(BLOCKS)
    moved_positions = jnp.moveaxis(blocks_now[0], 0, 1).reshape(3, BLOCKS, PART)
    moved_charges = blocks_now[1].reshape(BLOCKS, PART)
    moved_velocities = jnp.moveaxis(blocks_now[2], 0, 1).reshape(3, BLOCKS, PART)
    first_out = jnp.moveaxis(leaf_part, 0, 1).reshape(NCOEF, BLOCKS)
    second_out = jnp.moveaxis(parent_part, 0, 1).reshape(NCOEF, BLOCKS)
    return (moved_positions, moved_charges, moved_velocities, moved_leaves, first_out, second_out)
```

```python
import functools
import math

import jax
import jax.numpy as jnp
import numpy as np
from jax import lax
from jax.experimental import pallas as pl
from jax.experimental.pallas import tpu as pltpu
from jax.sharding import PartitionSpec as P

ORDER = 10
LEVEL = 7
CAP = 128
SLAB = 32
COMPS = 8
CHUNKS = 2
PER = COMPS // CHUNKS
MESH = pl.DeviceIdType.MESH

PHASES = (
    ("gx", (2, 1), 0),
    ("gy", (4, 2), 2),
    ("gy", (1,), 4),
    ("gz", (4, 2), 5),
    ("gz", (1,), 7),
)
SIZES = {"gx": 4, "gy": 8, "gz": 8}
STRIDES = {"gx": 64, "gy": 8, "gz": 1}
FRAMES = [(p, slot) for p, phase in enumerate(PHASES) for slot in range(2 ** len(phase[1]) - 1)]
LIST_BASE = 64
FP_BASE = 160
X_BASE = 128
FR_BASE = 32

TRIPLES = [
    (p, q, r)
    for p in range(ORDER + 1)
    for q in range(ORDER + 1 - p)
    for r in range(ORDER + 1 - p - q)
]
NCOEF = len(TRIPLES)
ROWS = 288


def bit_of(value, mask):
    return (value // mask) % 2


def flipped(value, mask):
    for one in (1, 2, 4):
        if mask & one:
            value = value + one - 2 * one * bit_of(value, one)
    return value


def pick(bit, one, zero):
    return bit * one + (1 - bit) * zero


def exchange(live, sends, leaves, positions, charges, velocities, final,
             list_a, list_b, frame_p, frame_r, frame_x, out, land,
             send_sem, recv_sem):
    where = {axis: lax.axis_index(axis) for axis in SIZES}

    def device(coords):
        return sum(coords[axis] * STRIDES[axis] for axis in SIZES)

    def moved(coords, axis, mask):
        return {**coords, axis: flipped(coords[axis], mask)}

    barrier = pltpu.get_barrier_semaphore()
    partners = 0
    for axis, masks, _ in PHASES:
        for mask in masks + ((sum(masks),) if len(masks) == 2 else ()):
            pl.semaphore_signal(
                barrier, inc=1, device_id={axis: flipped(where[axis], mask)}, device_id_type=MESH
            )
            partners += 1

    def section_step(coords, count, section, axis, mask):
        sent = sends[section, device(coords)]
        got = sends[section, device(moved(coords, axis, mask))]
        return sent, got, count - sent + got

    def start_count(coords, phase_now):
        count = live[device(coords)]
        for axis, masks, section in PHASES[:phase_now]:
            for step, mask in enumerate(masks):
                count = section_step(coords, count, section + step, axis, mask)[2]
        return count

    plans = []
    count = live[device(where)]
    for phase_now, (axis, masks, section) in enumerate(PHASES):
        plan = {}
        m1 = masks[0]
        a = bit_of(where[axis], m1)
        sent, got, count1 = section_step(where, count, section, axis, m1)
        kept = count - sent
        plan["start_a"] = pick(a, 0, kept)
        fs = pick(a, 0, kept)
        dl = pick(a, sent - got, 0)
        plan["got"] = got
        if len(masks) == 2:
            m2 = masks[1]
            b = bit_of(where[axis], m2)
            sent1, got1, count2 = section_step(where, count1, section + 1, axis, m2)
            kept1 = count1 - sent1
            start_b = pick(b, 0, kept1)
            plan["start_q"] = start_b + dl
            d1 = pick(b, sent1 - got1, 0)
            xs = pick(b, 0, kept1)
            plan["fs"] = fs - d1
            plan["list_off"] = dl + d1
            plan["xs"] = xs
            plan["xe"] = xs + got1
            other = moved(where, axis, m2)
            count_q = start_count(other, phase_now)
            sent_q, got_q, count1_q = section_step(other, count_q, section, axis, m1)
            fs_q = pick(a, 0, count_q - sent_q)
            start_bq = pick(b, count1_q - got1, 0)
            off_r = start_bq - fs_q
            plan["off_r"] = jnp.maximum(jnp.minimum(off_r, SLAB), -SLAB)
            plan["got_q"] = got_q
            count = count2
        else:
            plan["fs"] = fs
            plan["list_off"] = dl
            count = count1
        plan["fe"] = plan["fs"] + got
        plan["count"] = count
        plans.append(plan)

    for axis in range(3):
        list_a[axis, LIST_BASE : LIST_BASE + CAP] = positions[axis]
        list_a[4 + axis, LIST_BASE : LIST_BASE + CAP] = velocities[axis]
    list_a[3, LIST_BASE : LIST_BASE + CAP] = charges[...]
    list_a[7, LIST_BASE : LIST_BASE + CAP] = jnp.broadcast_to(
        leaves[...].astype(jnp.float32), (CAP, 128)
    ).T
    lists = (list_a, list_b)

    def transfers(p, j):
        axis, masks, _ = PHASES[p]
        rows = slice(PER * j, PER * (j + 1))
        todo = [(0, 0, masks[0])]
        if len(masks) == 2:
            todo += [(1, 1, masks[1]), (2, 0, masks[0] + masks[1])]
        copies = []
        for slot, source, mask in todo:
            at = FRAMES.index((p, slot)) * CHUNKS + j
            copies.append(
                pltpu.make_async_remote_copy(
                    src_ref=out.at[2 * p + source, rows],
                    dst_ref=land.at[3 * p + slot, rows],
                    send_sem=send_sem.at[at],
                    recv_sem=recv_sem.at[at],
                    device_id={axis: flipped(where[axis], mask)},
                    device_id_type=MESH,
                )
            )
        return copies

    started = {}

    def send(p, j):
        now, plan = lists[p % 2], plans[p]
        for k in range(PER * j, PER * (j + 1)):
            out[2 * p, k] = now[k, pl.ds(LIST_BASE + plan["start_a"], SLAB), :]
            if "start_q" in plan:
                out[2 * p + 1, k] = now[k, pl.ds(LIST_BASE + plan["start_q"], SLAB), :]
        started[p, j] = transfers(p, j)
        for copy in started[p, j]:
            copy.start()

    def receive(p, j):
        now, plan = lists[p % 2], plans[p]
        last = p == len(PHASES) - 1
        for copy in started[p, j]:
            copy.wait_recv()
        two = "start_q" in plan
        for k in range(PER * j, PER * (j + 1)):
            frame_p[k, FP_BASE : FP_BASE + SLAB] = land[3 * p, k]
            if two:
                frame_r[k, FR_BASE : FR_BASE + SLAB] = land[3 * p + 2, k]
        if two:
            row = lax.broadcasted_iota(jnp.int32, (SLAB, 128), 0) + plan["off_r"]
            from_r = (row >= 0) & (row < plan["got_q"])
            for k in range(PER * j, PER * (j + 1)):
                frame_x[k, X_BASE : X_BASE + SLAB] = jnp.where(
                    from_r,
                    frame_r[k, pl.ds(FR_BASE + plan["off_r"], SLAB), :],
                    land[3 * p + 1, k],
                )

        def tile(t, carry):
            base = t * 8
            row = lax.broadcasted_iota(jnp.int32, (8, 128), 0) + base
            from_p = (row >= plan["fs"]) & (row < plan["fe"])
            if two:
                from_x = (row >= plan["xs"]) & (row < plan["xe"])
            if last:
                full = row < plan["count"]
            for k in range(PER * j, PER * (j + 1)):
                value = jnp.where(
                    from_p,
                    frame_p[k, pl.ds(FP_BASE - plan["fs"] + base, 8), :],
                    now[k, pl.ds(LIST_BASE + plan["list_off"] + base, 8), :],
                )
                if two:
                    value = jnp.where(
                        from_x, frame_x[k, pl.ds(X_BASE - plan["xs"] + base, 8), :], value
                    )
                if last:
                    final[k, pl.ds(base, 8), :] = jnp.where(full, value, -1.0 if k == 7 else 0.0)
                else:
                    lists[(p + 1) % 2][k, pl.ds(LIST_BASE + base, 8), :] = value
            return carry

        lax.fori_loop(0, CAP // 8, tile, 0, unroll=True)

    pl.semaphore_wait(barrier, partners)
    for j in range(CHUNKS):
        send(0, j)
    for t in range(len(PHASES) + CHUNKS - 1):
        for j in reversed(range(CHUNKS)):
            p = t - j
            if 0 <= p < len(PHASES):
                receive(p, j)
                if p + 1 < len(PHASES):
                    send(p + 1, j)
    for copies in started.values():
        for copy in copies:
            copy.wait_send()


def shift_table():
    table = np.zeros((ROWS, ROWS), np.float32)
    for k, (p, q, r) in enumerate(TRIPLES):
        for j, (e, f, g) in enumerate(TRIPLES):
            if e <= p and f <= q and g <= r:
                table[k, j] = (
                    math.comb(p, e) * math.comb(q, f) * math.comb(r, g) * 0.5 ** (p + q + r)
                )
    return jnp.asarray(table, jnp.bfloat16)


def split3(value):
    high = value.astype(jnp.bfloat16)
    rest = value - high.astype(jnp.float32)
    middle = rest.astype(jnp.bfloat16)
    low = (rest - middle.astype(jnp.float32)).astype(jnp.bfloat16)
    return high, middle, low


def dot32(left, right):
    return jnp.dot(left, right, preferred_element_type=jnp.float32)


def moments(final, table, positions, charges, velocities, leaves, leaf_out, parent_out,
            u_ref, v_ref, w_ref, a_ref, b_ref, flip_ref, sign_ref, copy_sem):
    copies = [
        pltpu.make_async_copy(final.at[0:3], positions, copy_sem.at[0]),
        pltpu.make_async_copy(final.at[3], charges, copy_sem.at[1]),
        pltpu.make_async_copy(final.at[4:7], velocities, copy_sem.at[2]),
    ]
    for copy in copies:
        copy.start()
    leaf_rows = final[7]
    leaf_row = leaf_rows.T[0:8].astype(jnp.int32)
    leaves[...] = leaf_row[0:1]
    live_row = leaf_row >= 0
    leaf = jnp.where(live_row, leaf_row, 0)
    cells = []
    for axis_bit in (2, 1, 0):
        cell = jnp.zeros_like(leaf)
        for level in range(LEVEL):
            cell = cell + ((leaf >> (3 * level + axis_bit)) & 1) * 2**level
        cells.append(cell[0:1].astype(jnp.float32))
    for axis, ref in enumerate((u_ref, v_ref, w_ref)):
        ref[...] = 2.0 * (final[axis].T * float(2**LEVEL) - cells[axis]) - 1.0
    a_ref[...] = final[3].T * (1.0 / 16.0)
    flips = [
        jnp.where(((leaf >> bit) & 1)[0:1] == 1, 1.0, -1.0).astype(jnp.float32) for bit in (2, 1, 0)
    ]
    signs = {}
    for code in range(8):
        sign = jnp.ones((1, 128), jnp.float32)
        for axis in range(3):
            if code >> (2 - axis) & 1:
                sign = sign * flips[axis]
        signs[code] = sign
    flip_ref[280:288] = jnp.zeros((8, 128), jnp.float32)
    sign_ref[280:288] = jnp.zeros((8, 128), jnp.float32)
    step = 8
    k = 0
    for p in range(ORDER + 1):
        for q in range(ORDER + 1 - p):
            count = ORDER + 1 - p - q

            def body(g, sums, first=q == 0, more_q=q < ORDER - p, more_p=p < ORDER, count=count):
                sums = list(sums)
                for i in range(step):
                    rows = pl.ds((g * step + i) * 8, 8)
                    term = (a_ref if first else b_ref)[rows, :]
                    if more_q:
                        b_ref[rows, :] = term * v_ref[rows, :]
                    if first and more_p:
                        a_ref[rows, :] = term * u_ref[rows, :]
                    w = w_ref[rows, :]
                    for r in range(count):
                        sums[r] = sums[r] + term
                        if r + 1 < count:
                            term = term * w
                return tuple(sums)

            zero = jnp.zeros((8, 128), jnp.float32)
            sums = lax.fori_loop(0, 16 // step, body, (zero,) * count)
            for r in range(count):
                row = jnp.sum(sums[r], axis=0, keepdims=True)
                leaf_out[k : k + 1] = row
                sign = signs[(p & 1) << 2 | (q & 1) << 1 | (r & 1)]
                flip_ref[k : k + 1] = row * sign
                sign_ref[k : k + 1] = sign
                k += 1
    high, middle, low = split3(flip_ref[...])
    matrix = table[...]
    shifted = (dot32(matrix, low) + dot32(matrix, middle)) + dot32(matrix, high)
    shifted = shifted * sign_ref[...]
    leaf_col = leaf_rows.astype(jnp.int32)
    sibling = (
        ((leaf_col >> 3) == (leaf_row >> 3)[0:1]) & (leaf_col >= 0) & live_row[0:1]
    ).astype(jnp.float32).astype(jnp.bfloat16)
    high, middle, low = split3(shifted)
    total = (dot32(low, sibling) + dot32(middle, sibling)) + dot32(high, sibling)
    parent_out[...] = total[:NCOEF]
    for copy in copies:
        copy.wait()


def per_device(positions, charges, velocities, leaf_ids, live_counts, send_counts):
    vmem = pl.BlockSpec(memory_space=pltpu.VMEM)
    smem = pl.BlockSpec(memory_space=pltpu.SMEM)
    anywhere = pl.BlockSpec(memory_space=pl.ANY)
    f32 = jnp.float32
    copies = len(FRAMES) * CHUNKS
    final = pl.pallas_call(
        exchange,
        name="exchange",
        out_shape=jax.ShapeDtypeStruct((COMPS, CAP, 128), f32),
        in_specs=[smem, smem, vmem, vmem, vmem, vmem],
        out_specs=vmem,
        scratch_shapes=[
            pltpu.VMEM((COMPS, LIST_BASE + CAP + 64, 128), f32),
            pltpu.VMEM((COMPS, LIST_BASE + CAP + 64, 128), f32),
            pltpu.VMEM((COMPS, FP_BASE + CAP + 64, 128), f32),
            pltpu.VMEM((COMPS, FR_BASE + 2 * SLAB, 128), f32),
            pltpu.VMEM((COMPS, X_BASE + CAP, 128), f32),
            pltpu.VMEM((2 * len(PHASES), COMPS, SLAB, 128), f32),
            pltpu.VMEM((3 * len(PHASES), COMPS, SLAB, 128), f32),
            pltpu.SemaphoreType.DMA((copies,)),
            pltpu.SemaphoreType.DMA((copies,)),
        ],
        compiler_params=pltpu.CompilerParams(
            collective_id=0, has_side_effects=True, vmem_limit_bytes=24 * 2**20
        ),
    )(live_counts, send_counts, leaf_ids.reshape(1, CAP), positions, charges, velocities)

    square = pltpu.VMEM((CAP, 128), f32)
    outs = pl.pallas_call(
        moments,
        name="moments",
        out_shape=(
            jax.ShapeDtypeStruct((3, CAP, 128), f32),
            jax.ShapeDtypeStruct((CAP, 128), f32),
            jax.ShapeDtypeStruct((3, CAP, 128), f32),
            jax.ShapeDtypeStruct((1, CAP), jnp.int32),
            jax.ShapeDtypeStruct((NCOEF, CAP), f32),
            jax.ShapeDtypeStruct((NCOEF, CAP), f32),
        ),
        in_specs=[vmem, vmem],
        out_specs=(anywhere, anywhere, anywhere, vmem, vmem, vmem),
        scratch_shapes=[square] * 5
        + [
            pltpu.VMEM((ROWS, 128), f32),
            pltpu.VMEM((ROWS, 128), f32),
            pltpu.SemaphoreType.DMA((3,)),
        ],
        compiler_params=pltpu.CompilerParams(vmem_limit_bytes=16 * 2**20),
    )(final, shift_table())
    moved_positions, moved_charges, moved_velocities, moved_leaves, leaf_part, parent_part = outs
    return (
        moved_positions,
        moved_charges,
        moved_velocities,
        moved_leaves.reshape(CAP),
        leaf_part,
        parent_part,
    )


def solution(mesh):
    names = ("gx", "gy", "gz")
    in_specs = (P(None, names, None), P(names, None), P(None, names, None), P(names), P(), P())
    out_specs = (
        P(None, names, None),
        P(names, None),
        P(None, names, None),
        P(names),
        P(None, names),
        P(None, names),
    )
    return jax.shard_map(
        per_device, mesh=mesh, in_specs=in_specs, out_specs=out_specs, check_vma=False
    )
```

```python
import functools
import math

import jax
import jax.numpy as jnp
import numpy as np
from jax import lax
from jax.experimental import pallas as pl
from jax.experimental.pallas import tpu as pltpu
from jax.sharding import PartitionSpec as P

ORDER = 10
LEVEL = 7
CAP = 128
SLAB = 32
COMPS = 7
FRAME = SLAB * COMPS + 8
LEAF_ROWS = slice(SLAB * COMPS, FRAME)
CHUNKS = ((0, 2), (2, 5), (5, 7))
MESH = pl.DeviceIdType.MESH

PHASES = (
    ("gx", (2, 1), 0),
    ("gy", (4, 2), 2),
    ("gy", (1,), 4),
    ("gz", (4, 2), 5),
    ("gz", (1,), 7),
)
SIZES = {"gx": 4, "gy": 8, "gz": 8}
STRIDES = {"gx": 64, "gy": 8, "gz": 1}
FRAMES = [(p, slot) for p, phase in enumerate(PHASES) for slot in range(2 ** len(phase[1]) - 1)]
VMEM_LIMIT = 24 * 2**20
ORDER_OF_WORK = [
    (t - j, j)
    for t in range(len(PHASES) + len(CHUNKS) - 1)
    for j in reversed(range(len(CHUNKS)))
    if 0 <= t - j < len(PHASES)
]
LIST_BASE = 64
FP_BASE = 160
X_BASE = 128
FR_BASE = 32

TRIPLES = [
    (p, q, r)
    for p in range(ORDER + 1)
    for q in range(ORDER + 1 - p)
    for r in range(ORDER + 1 - p - q)
]
NCOEF = len(TRIPLES)
ROWS = 288


def bits_of(value):
    high = jnp.where(value >= 4, 1, 0)
    rest = value - 4 * high
    middle = jnp.where(rest >= 2, 1, 0)
    return {4: high, 2: middle, 1: rest - 2 * middle}


def pick(bit, one, zero):
    return bit * one + (1 - bit) * zero


def exchange(live_hbm, sends_hbm, leaves_hbm, positions, charges, velocities, final, leaf_final,
             live, sends, leaves, list_a, list_b, frame_p, frame_r, frame_x, out, land,
             load_sem, send_sem, recv_sem):
    where = {axis: lax.axis_index(axis) for axis in SIZES}
    bits = {axis: bits_of(where[axis]) for axis in SIZES}
    me = sum(where[axis] * STRIDES[axis] for axis in SIZES)

    def step_of(axis, mask):
        return sum(m - 2 * m * bits[axis][m] for m in (4, 2, 1) if mask & m)

    def peer(axis, mask):
        return {axis: where[axis] + step_of(axis, mask)}

    def device(flips):
        return me + sum(step_of(axis, mask) * STRIDES[axis] for axis, mask in flips)

    def moved(flips, axis, mask):
        return flips ^ {(axis, mask)}

    barrier = pltpu.get_barrier_semaphore()
    partners = 0
    for axis, masks, _ in PHASES:
        for mask in masks + ((sum(masks),) if len(masks) == 2 else ()):
            pl.semaphore_signal(
                barrier, inc=1, device_id=peer(axis, mask), device_id_type=MESH
            )
            partners += 1
    lists = (list_a, list_b)
    body = slice(LIST_BASE, LIST_BASE + CAP)
    pairs = [(live_hbm, live), (sends_hbm, sends), (leaves_hbm, leaves)]
    pairs += [(positions.at[k], list_a.at[k, body]) for k in range(3)]
    pairs += [(charges, list_a.at[3, body])]
    pairs += [(velocities.at[k], list_a.at[4 + k, body]) for k in range(3)]
    loads = [
        pltpu.make_async_copy(source, target, load_sem.at[k])
        for k, (source, target) in enumerate(pairs)
    ]
    for load in loads:
        load.start()
    for load in loads[:2]:
        load.wait()

    def section_step(coords, count, section, axis, mask):
        sent = sends[section, device(coords)]
        got = sends[section, device(moved(coords, axis, mask))]
        return sent, got, count - sent + got

    def start_count(coords, phase_now):
        count = live[device(coords)]
        for axis, masks, section in PHASES[:phase_now]:
            for step, mask in enumerate(masks):
                count = section_step(coords, count, section + step, axis, mask)[2]
        return count

    plans = []
    here = frozenset()
    count = live[device(here)]
    for phase_now, (axis, masks, section) in enumerate(PHASES):
        plan = {}
        m1 = masks[0]
        a = bits[axis][m1]
        sent, got, count1 = section_step(here, count, section, axis, m1)
        kept = count - sent
        plan["start_a"] = pick(a, 0, kept)
        fs = pick(a, 0, kept)
        dl = pick(a, sent - got, 0)
        if len(masks) == 2:
            m2 = masks[1]
            b = bits[axis][m2]
            sent1, got1, count2 = section_step(here, count1, section + 1, axis, m2)
            kept1 = count1 - sent1
            start_b = pick(b, 0, kept1)
            plan["start_q"] = start_b + dl
            d1 = pick(b, sent1 - got1, 0)
            xs = pick(b, 0, kept1)
            plan["fs"] = fs - d1
            plan["list_off"] = dl + d1
            plan["xs"] = xs
            plan["xe"] = xs + got1
            other = moved(here, axis, m2)
            count_q = start_count(other, phase_now)
            sent_q, got_q, count1_q = section_step(other, count_q, section, axis, m1)
            fs_q = pick(a, 0, count_q - sent_q)
            start_bq = pick(b, count1_q - got1, 0)
            off_r = start_bq - fs_q
            plan["off_r"] = jnp.maximum(jnp.minimum(off_r, SLAB), -SLAB)
            plan["got_q"] = got_q
            count = count2
        else:
            plan["fs"] = fs
            plan["list_off"] = dl
            count = count1
        plan["fe"] = plan["fs"] + got
        plan["count"] = count
        plans.append(plan)

    def transfers(p, j):
        axis, masks, _ = PHASES[p]
        first, end = CHUNKS[j]
        rows = slice(SLAB * first, SLAB * end + (8 if end == COMPS else 0))
        todo = [(0, 0, masks[0])]
        if len(masks) == 2:
            todo += [(1, 1, masks[1]), (2, 0, masks[0] + masks[1])]
        copies = []
        for slot, source, mask in todo:
            at = FRAMES.index((p, slot)) * len(CHUNKS) + j
            copies.append(
                pltpu.make_async_remote_copy(
                    src_ref=out.at[2 * p + source, rows],
                    dst_ref=land.at[3 * p + slot, rows],
                    send_sem=send_sem.at[at],
                    recv_sem=recv_sem.at[at],
                    device_id=peer(axis, mask),
                    device_id_type=MESH,
                )
            )
        return copies

    started = {}
    leaf_list = {}

    def to_left(row, amount):
        return pltpu.roll(row, (4 * 128 - amount) % 128, 1)

    def send(p, j):
        now, plan = lists[p % 2], plans[p]
        first, end = CHUNKS[j]
        two = "start_q" in plan
        for k in range(first, end):
            rows = slice(SLAB * k, SLAB * (k + 1))
            out[2 * p, rows] = now[k, pl.ds(LIST_BASE + plan["start_a"], SLAB), :]
            if two:
                out[2 * p + 1, rows] = now[k, pl.ds(LIST_BASE + plan["start_q"], SLAB), :]
        if end == COMPS:
            out[2 * p, LEAF_ROWS] = to_left(leaf_list[p], plan["start_a"])
            if two:
                out[2 * p + 1, LEAF_ROWS] = to_left(leaf_list[p], plan["start_q"])
        started[p, j] = transfers(p, j)
        for copy in started[p, j]:
            copy.start()

    def receive(p, j):
        now, plan = lists[p % 2], plans[p]
        last = p == len(PHASES) - 1
        first, end = CHUNKS[j]
        for copy in started[p, j]:
            copy.wait_recv()
        two = "start_q" in plan
        for k in range(first, end):
            rows = slice(SLAB * k, SLAB * (k + 1))
            frame_p[k, FP_BASE : FP_BASE + SLAB] = land[3 * p, rows]
            if two:
                frame_r[k, FR_BASE : FR_BASE + SLAB] = land[3 * p + 2, rows]
        if two:
            row = lax.broadcasted_iota(jnp.int32, (SLAB, 128), 0) + plan["off_r"]
            from_r = (row >= 0) & (row < plan["got_q"])
            for k in range(first, end):
                frame_x[k, X_BASE : X_BASE + SLAB] = jnp.where(
                    from_r,
                    frame_r[k, pl.ds(FR_BASE + plan["off_r"], SLAB), :],
                    land[3 * p + 1, SLAB * k : SLAB * (k + 1)],
                )

        def tile(t, carry):
            base = t * 8
            row = lax.broadcasted_iota(jnp.int32, (8, 128), 0) + base
            from_p = (row >= plan["fs"]) & (row < plan["fe"])
            if two:
                from_x = (row >= plan["xs"]) & (row < plan["xe"])
            if last:
                full = row < plan["count"]
            for k in range(first, end):
                value = jnp.where(
                    from_p,
                    frame_p[k, pl.ds(FP_BASE - plan["fs"] + base, 8), :],
                    now[k, pl.ds(LIST_BASE + plan["list_off"] + base, 8), :],
                )
                if two:
                    value = jnp.where(
                        from_x, frame_x[k, pl.ds(X_BASE - plan["xs"] + base, 8), :], value
                    )
                if last:
                    final[k, pl.ds(base, 8), :] = jnp.where(full, value, 0.0)
                else:
                    lists[(p + 1) % 2][k, pl.ds(LIST_BASE + base, 8), :] = value
            return carry

        lax.fori_loop(0, CAP // 8, tile, 0, unroll=True)
        if end == COMPS:
            lane = lax.broadcasted_iota(jnp.int32, (8, 128), 1)
            value = jnp.where(
                (lane >= plan["fs"]) & (lane < plan["fe"]),
                to_left(land[3 * p, LEAF_ROWS], -plan["fs"]),
                to_left(leaf_list[p], plan["list_off"]),
            )
            if two:
                at = lane + plan["off_r"]
                second = jnp.where(
                    (at >= 0) & (at < plan["got_q"]),
                    to_left(land[3 * p + 2, LEAF_ROWS], plan["off_r"]),
                    land[3 * p + 1, LEAF_ROWS],
                )
                value = jnp.where(
                    (lane >= plan["xs"]) & (lane < plan["xe"]), to_left(second, -plan["xs"]), value
                )
            if last:
                leaf_final[...] = jnp.where(lane < plan["count"], value, -1.0).astype(jnp.int32)
            else:
                leaf_list[p + 1] = value

    for load in loads[2:]:
        load.wait()
    leaf_list[0] = jnp.broadcast_to(leaves[...], (8, 128)).astype(jnp.float32)
    pl.semaphore_wait(barrier, partners)
    for j in range(len(CHUNKS)):
        send(0, j)
    for p, j in ORDER_OF_WORK:
        receive(p, j)
        if p + 1 < len(PHASES):
            send(p + 1, j)
    for copies in started.values():
        for copy in copies:
            copy.wait_send()


def shift_table():
    table = np.zeros((ROWS, ROWS), np.float32)
    for k, (p, q, r) in enumerate(TRIPLES):
        for j, (e, f, g) in enumerate(TRIPLES):
            if e <= p and f <= q and g <= r:
                table[k, j] = (
                    math.comb(p, e) * math.comb(q, f) * math.comb(r, g) * 0.5 ** (p + q + r)
                )
    return jnp.asarray(table, jnp.bfloat16)


def split3(value):
    high = value.astype(jnp.bfloat16)
    rest = value - high.astype(jnp.float32)
    middle = rest.astype(jnp.bfloat16)
    low = (rest - middle.astype(jnp.float32)).astype(jnp.bfloat16)
    return high, middle, low


def dot32(left, right):
    return jnp.dot(left, right, preferred_element_type=jnp.float32)


def moments(final, leaf_final, table, positions, charges, velocities, leaves, leaf_out, parent_out,
            u_ref, v_ref, w_ref, a_ref, b_ref, flip_ref, sign_ref, copy_sem):
    copies = [
        pltpu.make_async_copy(final.at[0:3], positions, copy_sem.at[0]),
        pltpu.make_async_copy(final.at[3], charges, copy_sem.at[1]),
        pltpu.make_async_copy(final.at[4:7], velocities, copy_sem.at[2]),
    ]
    for copy in copies:
        copy.start()
    leaf_row = leaf_final[...]
    leaves[...] = leaf_row[0:1]
    live_row = leaf_row >= 0
    leaf = jnp.where(live_row, leaf_row, 0)
    cells = []
    for axis_bit in (2, 1, 0):
        cell = jnp.zeros_like(leaf)
        for level in range(LEVEL):
            cell = cell + ((leaf >> (3 * level + axis_bit)) & 1) * 2**level
        cells.append(cell[0:1].astype(jnp.float32))
    for axis, ref in enumerate((u_ref, v_ref, w_ref)):
        ref[...] = 2.0 * (final[axis].T * float(2**LEVEL) - cells[axis]) - 1.0
    a_ref[...] = final[3].T * (1.0 / 16.0)
    flips = [
        jnp.where(((leaf >> bit) & 1)[0:1] == 1, 1.0, -1.0).astype(jnp.float32) for bit in (2, 1, 0)
    ]
    signs = {}
    for code in range(8):
        sign = jnp.ones((1, 128), jnp.float32)
        for axis in range(3):
            if code >> (2 - axis) & 1:
                sign = sign * flips[axis]
        signs[code] = sign
    flip_ref[280:288] = jnp.zeros((8, 128), jnp.float32)
    sign_ref[280:288] = jnp.zeros((8, 128), jnp.float32)
    step = 8
    k = 0
    for p in range(ORDER + 1):
        for q in range(ORDER + 1 - p):
            count = ORDER + 1 - p - q

            def body(g, sums, first=q == 0, more_q=q < ORDER - p, more_p=p < ORDER, count=count):
                sums = list(sums)
                for i in range(step):
                    rows = pl.ds((g * step + i) * 8, 8)
                    term = (a_ref if first else b_ref)[rows, :]
                    if more_q:
                        b_ref[rows, :] = term * v_ref[rows, :]
                    if first and more_p:
                        a_ref[rows, :] = term * u_ref[rows, :]
                    w = w_ref[rows, :]
                    for r in range(count):
                        sums[r] = sums[r] + term
                        if r + 1 < count:
                            term = term * w
                return tuple(sums)

            zero = jnp.zeros((8, 128), jnp.float32)
            sums = lax.fori_loop(0, 16 // step, body, (zero,) * count)
            for r in range(count):
                row = jnp.sum(sums[r], axis=0, keepdims=True)
                leaf_out[k : k + 1] = row
                sign = signs[(p & 1) << 2 | (q & 1) << 1 | (r & 1)]
                flip_ref[k : k + 1] = row * sign
                sign_ref[k : k + 1] = sign
                k += 1
    high, middle, low = split3(flip_ref[...])
    matrix = table[...]
    shifted = (dot32(matrix, low) + dot32(matrix, middle)) + dot32(matrix, high)
    shifted = shifted * sign_ref[...]
    leaf_col = jnp.broadcast_to(leaf_row[0:1].astype(jnp.float32), (CAP, 128)).T.astype(jnp.int32)
    sibling = (
        ((leaf_col >> 3) == (leaf_row >> 3)[0:1]) & (leaf_col >= 0) & live_row[0:1]
    ).astype(jnp.float32).astype(jnp.bfloat16)
    high, middle, low = split3(shifted)
    total = (dot32(low, sibling) + dot32(middle, sibling)) + dot32(high, sibling)
    parent_out[...] = total[:NCOEF]
    for copy in copies:
        copy.wait()


def per_device(positions, charges, velocities, leaf_ids, live_counts, send_counts):
    vmem = pl.BlockSpec(memory_space=pltpu.VMEM)
    smem = pl.BlockSpec(memory_space=pltpu.SMEM)
    anywhere = pl.BlockSpec(memory_space=pl.ANY)
    f32 = jnp.float32
    copies = len(FRAMES) * len(CHUNKS)
    final, leaf_final = pl.pallas_call(
        exchange,
        name="exchange",
        out_shape=(
            jax.ShapeDtypeStruct((COMPS, CAP, 128), f32),
            jax.ShapeDtypeStruct((8, CAP), jnp.int32),
        ),
        in_specs=[anywhere] * 6,
        out_specs=(vmem, vmem),
        scratch_shapes=[
            pltpu.SMEM((256,), jnp.int32),
            pltpu.SMEM((8, 256), jnp.int32),
            pltpu.VMEM((1, CAP), jnp.int32),
            pltpu.VMEM((COMPS, LIST_BASE + CAP + 64, 128), f32),
            pltpu.VMEM((COMPS, LIST_BASE + CAP + 64, 128), f32),
            pltpu.VMEM((COMPS, FP_BASE + CAP + 64, 128), f32),
            pltpu.VMEM((COMPS, FR_BASE + 2 * SLAB, 128), f32),
            pltpu.VMEM((COMPS, X_BASE + CAP, 128), f32),
            pltpu.VMEM((2 * len(PHASES), FRAME, 128), f32),
            pltpu.VMEM((3 * len(PHASES), FRAME, 128), f32),
            pltpu.SemaphoreType.DMA((3 + COMPS,)),
            pltpu.SemaphoreType.DMA((copies,)),
            pltpu.SemaphoreType.DMA((copies,)),
        ],
        compiler_params=pltpu.CompilerParams(
            collective_id=0, has_side_effects=True, vmem_limit_bytes=VMEM_LIMIT
        ),
    )(*(pltpu.with_memory_space_constraint(x, pltpu.HBM) for x in (live_counts, send_counts, leaf_ids.reshape(1, CAP), positions, charges, velocities)))

    square = pltpu.VMEM((CAP, 128), f32)
    outs = pl.pallas_call(
        moments,
        name="moments",
        out_shape=(
            jax.ShapeDtypeStruct((3, CAP, 128), f32),
            jax.ShapeDtypeStruct((CAP, 128), f32),
            jax.ShapeDtypeStruct((3, CAP, 128), f32),
            jax.ShapeDtypeStruct((1, CAP), jnp.int32),
            jax.ShapeDtypeStruct((NCOEF, CAP), f32),
            jax.ShapeDtypeStruct((NCOEF, CAP), f32),
        ),
        in_specs=[vmem, vmem, vmem],
        out_specs=(anywhere, anywhere, anywhere, vmem, vmem, vmem),
        scratch_shapes=[square] * 5
        + [
            pltpu.VMEM((ROWS, 128), f32),
            pltpu.VMEM((ROWS, 128), f32),
            pltpu.SemaphoreType.DMA((3,)),
        ],
        compiler_params=pltpu.CompilerParams(vmem_limit_bytes=16 * 2**20),
    )(final, leaf_final, shift_table())
    moved_positions, moved_charges, moved_velocities, moved_leaves, leaf_part, parent_part = outs
    return (
        moved_positions,
        moved_charges,
        moved_velocities,
        moved_leaves.reshape(CAP),
        leaf_part,
        parent_part,
    )


def solution(mesh):
    names = ("gx", "gy", "gz")
    in_specs = (P(None, names, None), P(names, None), P(None, names, None), P(names), P(), P())
    out_specs = (
        P(None, names, None),
        P(names, None),
        P(None, names, None),
        P(names),
        P(None, names),
        P(None, names),
    )
    return jax.shard_map(
        per_device, mesh=mesh, in_specs=in_specs, out_specs=out_specs, check_vma=False
    )
```

```python
import functools
import math

import jax
import jax.numpy as jnp
import numpy as np
from jax import lax
from jax.experimental import pallas as pl
from jax.experimental.pallas import tpu as pltpu
from jax.sharding import PartitionSpec as P

ORDER = 10
LEVEL = 7
CAP = 128
SLAB = 32
COMPS = 7
FRAME = SLAB * COMPS + 8
LEAF_ROWS = slice(SLAB * 4, SLAB * 4 + 8)
CHUNKS = ((0, 1), (1, 2), (2, 4), (4, 6), (6, 7))
MESH = pl.DeviceIdType.MESH

PHASES = (
    ("gx", (2, 1), 0),
    ("gy", (4, 2), 2),
    ("gy", (1,), 4),
    ("gz", (4, 2), 5),
    ("gz", (1,), 7),
)
SIZES = {"gx": 4, "gy": 8, "gz": 8}
STRIDES = {"gx": 64, "gy": 8, "gz": 1}
FRAMES = [(p, slot) for p, phase in enumerate(PHASES) for slot in range(2 ** len(phase[1]) - 1)]
VMEM_LIMIT = 24 * 2**20
ORDER_OF_WORK = (
    [(0, 0), (0, 1), (0, 2), (0, 3), (0, 4), (1, 0), (1, 1), (2, 0), (2, 1), (1, 2), (1, 3), (2, 2)]
    + [(1, 4), (2, 3), (2, 4), (3, 0), (3, 1), (3, 2), (4, 0), (4, 1), (3, 3), (4, 2), 0, (3, 4), 1]
    + [2, 3, (4, 3), (4, 4)]
)
LIST_BASE = 64
FP_BASE = 160
X_BASE = 128
FR_BASE = 32

TRIPLES = [
    (p, q, r)
    for p in range(ORDER + 1)
    for q in range(ORDER + 1 - p)
    for r in range(ORDER + 1 - p - q)
]
NCOEF = len(TRIPLES)
ROWS = 288


def bits_of(value):
    high = jnp.where(value >= 4, 1, 0)
    rest = value - 4 * high
    middle = jnp.where(rest >= 2, 1, 0)
    return {4: high, 2: middle, 1: rest - 2 * middle}


def rows_of(first, end):
    return slice(SLAB * first + 8 * (first >= 4), SLAB * end + 8 * (end >= 4))


def frame_rows(k):
    start = SLAB * k + 8 * (k >= 4)
    return slice(start, start + SLAB)


def pick(bit, one, zero):
    return bit * one + (1 - bit) * zero


def exchange(live_hbm, sends_hbm, leaves_hbm, positions, charges, velocities, table_hbm,
             final, leaf_final, leaf_out, parent_out,
             live, sends, leaves, list_a, list_b, frame_p, frame_r, frame_x, out, land,
             table, u_ref, v_ref, w_ref, a_ref, b_ref, flip_ref, sign_ref,
             load_sem, send_sem, recv_sem, vouched):
    moment_refs = (leaf_out, parent_out, u_ref, v_ref, w_ref, a_ref, b_ref, flip_ref, sign_ref)
    where = {axis: lax.axis_index(axis) for axis in SIZES}
    bits = {axis: bits_of(where[axis]) for axis in SIZES}
    me = sum(where[axis] * STRIDES[axis] for axis in SIZES)

    def step_of(axis, mask):
        return sum(m - 2 * m * bits[axis][m] for m in (4, 2, 1) if mask & m)

    def peer(axis, mask):
        return {axis: where[axis] + step_of(axis, mask)}

    def device(flips):
        return me + sum(step_of(axis, mask) * STRIDES[axis] for axis, mask in flips)

    def moved(flips, axis, mask):
        return flips ^ {(axis, mask)}

    barrier = pltpu.get_barrier_semaphore()
    partners = 0
    for axis, masks, _ in PHASES:
        for mask in masks + ((sum(masks),) if len(masks) == 2 else ()):
            if (axis, mask) == ("gz", 4):
                continue
            pl.semaphore_signal(
                barrier, inc=1, device_id=peer(axis, mask), device_id_type=MESH
            )
            partners += 1
    lists = (list_a, list_b)
    body = slice(LIST_BASE, LIST_BASE + CAP)
    pairs = [(live_hbm, live), (sends_hbm, sends), (leaves_hbm, leaves)]
    pairs += [(positions.at[k], list_a.at[k, body]) for k in range(3)]
    pairs += [(charges, list_a.at[3, body])]
    pairs += [(velocities.at[k], list_a.at[4 + k, body]) for k in range(3)]
    pairs += [(table_hbm, table)]
    loads = [
        pltpu.make_async_copy(source, target, load_sem.at[k])
        for k, (source, target) in enumerate(pairs)
    ]
    for load in loads:
        load.start()
    for load in loads[:2]:
        load.wait()

    def section_step(coords, count, section, axis, mask):
        sent = sends[section, device(coords)]
        got = sends[section, device(moved(coords, axis, mask))]
        return sent, got, count - sent + got

    def start_count(coords, phase_now):
        count = live[device(coords)]
        for axis, masks, section in PHASES[:phase_now]:
            for step, mask in enumerate(masks):
                count = section_step(coords, count, section + step, axis, mask)[2]
        return count

    plans = []
    here = frozenset()
    count = live[device(here)]
    for phase_now, (axis, masks, section) in enumerate(PHASES):
        plan = {}
        m1 = masks[0]
        a = bits[axis][m1]
        sent, got, count1 = section_step(here, count, section, axis, m1)
        kept = count - sent
        plan["start_a"] = pick(a, 0, kept)
        fs = pick(a, 0, kept)
        dl = pick(a, sent - got, 0)
        if len(masks) == 2:
            m2 = masks[1]
            b = bits[axis][m2]
            sent1, got1, count2 = section_step(here, count1, section + 1, axis, m2)
            kept1 = count1 - sent1
            start_b = pick(b, 0, kept1)
            plan["start_q"] = start_b + dl
            d1 = pick(b, sent1 - got1, 0)
            xs = pick(b, 0, kept1)
            plan["fs"] = fs - d1
            plan["list_off"] = dl + d1
            plan["xs"] = xs
            plan["xe"] = xs + got1
            other = moved(here, axis, m2)
            count_q = start_count(other, phase_now)
            sent_q, got_q, count1_q = section_step(other, count_q, section, axis, m1)
            fs_q = pick(a, 0, count_q - sent_q)
            start_bq = pick(b, count1_q - got1, 0)
            off_r = start_bq - fs_q
            plan["off_r"] = jnp.maximum(jnp.minimum(off_r, SLAB), -SLAB)
            plan["got_q"] = got_q
            count = count2
        else:
            plan["fs"] = fs
            plan["list_off"] = dl
            count = count1
        plan["fe"] = plan["fs"] + got
        plan["count"] = count
        plans.append(plan)

    def transfers(p, j):
        axis, masks, _ = PHASES[p]
        first, end = CHUNKS[j]
        rows = rows_of(first, end)
        todo = [(0, 0, masks[0])]
        if len(masks) == 2:
            todo += [(1, 1, masks[1]), (2, 0, masks[0] + masks[1])]
        copies = []
        for slot, source, mask in todo:
            at = FRAMES.index((p, slot)) * len(CHUNKS) + j
            copies.append(
                pltpu.make_async_remote_copy(
                    src_ref=out.at[2 * p + source, rows],
                    dst_ref=land.at[3 * p + slot, rows],
                    send_sem=send_sem.at[at],
                    recv_sem=recv_sem.at[at],
                    device_id=peer(axis, mask),
                    device_id_type=MESH,
                )
            )
        return copies

    started = {}
    leaf_list = {}

    def to_left(row, amount):
        return pltpu.roll(row, (4 * 128 - amount) % 128, 1)

    def send(p, j):
        now, plan = lists[p % 2], plans[p]
        first, end = CHUNKS[j]
        two = "start_q" in plan
        for k in range(first, end):
            rows = frame_rows(k)
            out[2 * p, rows] = now[k, pl.ds(LIST_BASE + plan["start_a"], SLAB), :]
            if two:
                out[2 * p + 1, rows] = now[k, pl.ds(LIST_BASE + plan["start_q"], SLAB), :]
        if end == 4:
            out[2 * p, LEAF_ROWS] = to_left(leaf_list[p], plan["start_a"])
            if two:
                out[2 * p + 1, LEAF_ROWS] = to_left(leaf_list[p], plan["start_q"])
        started[p, j] = transfers(p, j)
        for copy in started[p, j]:
            copy.start()

    def receive(p, j):
        now, plan = lists[p % 2], plans[p]
        last = p == len(PHASES) - 1
        first, end = CHUNKS[j]
        for copy in started[p, j]:
            copy.wait_recv()
        two = "start_q" in plan
        for k in range(first, end):
            rows = frame_rows(k)
            frame_p[k, FP_BASE : FP_BASE + SLAB] = land[3 * p, rows]
            if two:
                frame_r[k, FR_BASE : FR_BASE + SLAB] = land[3 * p + 2, rows]
        if two:
            row = lax.broadcasted_iota(jnp.int32, (SLAB, 128), 0) + plan["off_r"]
            from_r = (row >= 0) & (row < plan["got_q"])
            for k in range(first, end):
                frame_x[k, X_BASE : X_BASE + SLAB] = jnp.where(
                    from_r,
                    frame_r[k, pl.ds(FR_BASE + plan["off_r"], SLAB), :],
                    land[3 * p + 1, frame_rows(k)],
                )

        def tile(t, carry):
            base = t * 8
            row = lax.broadcasted_iota(jnp.int32, (8, 128), 0) + base
            from_p = (row >= plan["fs"]) & (row < plan["fe"])
            if two:
                from_x = (row >= plan["xs"]) & (row < plan["xe"])
            if last:
                full = row < plan["count"]
            for k in range(first, end):
                value = jnp.where(
                    from_p,
                    frame_p[k, pl.ds(FP_BASE - plan["fs"] + base, 8), :],
                    now[k, pl.ds(LIST_BASE + plan["list_off"] + base, 8), :],
                )
                if two:
                    value = jnp.where(
                        from_x, frame_x[k, pl.ds(X_BASE - plan["xs"] + base, 8), :], value
                    )
                if last:
                    final[k, pl.ds(base, 8), :] = jnp.where(full, value, 0.0)
                else:
                    lists[(p + 1) % 2][k, pl.ds(LIST_BASE + base, 8), :] = value
            return carry

        lax.fori_loop(0, CAP // 8, tile, 0, unroll=True)
        if end == 4:
            lane = lax.broadcasted_iota(jnp.int32, (8, 128), 1)
            value = jnp.where(
                (lane >= plan["fs"]) & (lane < plan["fe"]),
                to_left(land[3 * p, LEAF_ROWS], -plan["fs"]),
                to_left(leaf_list[p], plan["list_off"]),
            )
            if two:
                at = lane + plan["off_r"]
                second = jnp.where(
                    (at >= 0) & (at < plan["got_q"]),
                    to_left(land[3 * p + 2, LEAF_ROWS], plan["off_r"]),
                    land[3 * p + 1, LEAF_ROWS],
                )
                value = jnp.where(
                    (lane >= plan["xs"]) & (lane < plan["xe"]), to_left(second, -plan["xs"]), value
                )
            if last:
                leaf_final[...] = jnp.where(lane < plan["count"], value, -1.0).astype(jnp.int32)
            else:
                leaf_list[p + 1] = value

    for load in loads[2:]:
        load.wait()
    leaf_list[0] = jnp.broadcast_to(leaves[...], (8, 128)).astype(jnp.float32)
    pl.semaphore_wait(barrier, partners)
    for j in range(len(CHUNKS)):
        send(0, j)
    pl.semaphore_signal(vouched, inc=1, device_id=peer("gz", 6), device_id_type=MESH)
    moments = moment_pieces(final, leaf_final, table, *moment_refs)
    for work in ORDER_OF_WORK:
        if isinstance(work, int):
            moments[work]()
            continue
        p, j = work
        receive(p, j)
        if p + 1 < len(PHASES):
            if (p + 1, j) == (3, 0):
                pl.semaphore_wait(vouched, 1)
            send(p + 1, j)
    for copies in started.values():
        for copy in copies:
            copy.wait_send()


def shift_table():
    table = np.zeros((ROWS, ROWS), np.float32)
    for k, (p, q, r) in enumerate(TRIPLES):
        for j, (e, f, g) in enumerate(TRIPLES):
            if e <= p and f <= q and g <= r:
                table[k, j] = (
                    math.comb(p, e) * math.comb(q, f) * math.comb(r, g) * 0.5 ** (p + q + r)
                )
    return jnp.asarray(table, jnp.bfloat16)


def split3(value):
    high = value.astype(jnp.bfloat16)
    rest = value - high.astype(jnp.float32)
    middle = rest.astype(jnp.bfloat16)
    low = (rest - middle.astype(jnp.float32)).astype(jnp.bfloat16)
    return high, middle, low


def dot32(left, right):
    return jnp.dot(left, right, preferred_element_type=jnp.float32)


def packed_sums(parts):
    row = lax.broadcasted_iota(jnp.int32, (8, 128), 0)
    low = row < 4
    parts = [
        jnp.where(low, one, two) + pltpu.roll(jnp.where(low, two, one), 4, 0)
        for one, two in zip(parts[:4], parts[4:])
    ]
    for half in (2, 1):
        low = row % (2 * half) < half
        parts = [
            jnp.where(low, one, two)
            + jnp.where(low, pltpu.roll(one, 8 - half, 0), pltpu.roll(two, half, 0))
            for one, two in zip(parts[:half], parts[half:])
        ]
    return parts[0]


def moment_pieces(final, leaf_final, table, leaf_out, parent_out,
                  u_ref, v_ref, w_ref, a_ref, b_ref, flip_ref, sign_ref):
    state = {"sums": [], "k": 0}
    step = 8

    def begin():
        leaf_row = leaf_final[...]
        leaf = jnp.where(leaf_row >= 0, leaf_row, 0)
        cells = []
        for axis_bit in (2, 1, 0):
            cell = jnp.zeros_like(leaf)
            for level in range(LEVEL):
                cell = cell + ((leaf >> (3 * level + axis_bit)) & 1) * 2**level
            cells.append(cell[0:1].astype(jnp.float32))
        for axis, ref in enumerate((u_ref, v_ref, w_ref)):
            ref[...] = 2.0 * (final[axis].T * float(2**LEVEL) - cells[axis]) - 1.0
        a_ref[...] = final[3].T * (1.0 / 16.0)
        state["flips"] = [
            jnp.where(((leaf >> bit) & 1) == 1, 1.0, -1.0).astype(jnp.float32) for bit in (2, 1, 0)
        ]

    def store(parts, first):
        parts = parts + [jnp.zeros((8, 128), jnp.float32)] * (8 - len(parts))
        rows = packed_sums(parts)
        row = lax.broadcasted_iota(jnp.int32, (8, 128), 0)
        sign = jnp.ones((8, 128), jnp.float32)
        for axis in range(3):
            odd = sum(
                (TRIPLES[first + i][axis] & 1) << i for i in range(8) if first + i < NCOEF
            )
            if odd:
                sign = sign * jnp.where((odd >> row) & 1 == 1, state["flips"][axis], 1.0)
        count = min(8, NCOEF - first)
        leaf_out[first : first + count] = rows[:count]
        flip_ref[first : first + 8] = rows * sign
        sign_ref[first : first + 8] = sign

    def sums_of(orders):
        for p in orders:
            for q in range(ORDER + 1 - p):
                count = ORDER + 1 - p - q

                def body(g, sums, first=q == 0, more_q=q < ORDER - p, more_p=p < ORDER, count=count):
                    sums = list(sums)
                    for i in range(step):
                        rows = pl.ds((g * step + i) * 8, 8)
                        term = (a_ref if first else b_ref)[rows, :]
                        if more_q:
                            b_ref[rows, :] = term * v_ref[rows, :]
                        if first and more_p:
                            a_ref[rows, :] = term * u_ref[rows, :]
                        w = w_ref[rows, :]
                        for r in range(count):
                            sums[r] = sums[r] + term
                            if r + 1 < count:
                                term = term * w
                    return tuple(sums)

                zero = jnp.zeros((8, 128), jnp.float32)
                state["sums"] += list(lax.fori_loop(0, 16 // step, body, (zero,) * count))
                while len(state["sums"]) >= 8:
                    store(state["sums"][:8], state["k"])
                    state["sums"] = state["sums"][8:]
                    state["k"] += 8
        if orders[-1] == ORDER:
            store(state["sums"], state["k"])

    def parents():
        high, middle, low = split3(flip_ref[...])
        matrix = table[...]
        shifted = (dot32(matrix, low) + dot32(matrix, middle)) + dot32(matrix, high)
        shifted = shifted * sign_ref[...]
        leaf_row = leaf_final[0:1]
        leaf_col = (
            jnp.broadcast_to(leaf_row.astype(jnp.float32), (CAP, 128)).T.astype(jnp.int32)
        )
        sibling = (
            ((leaf_col >> 3) == (leaf_row >> 3)) & (leaf_col >= 0) & (leaf_row >= 0)
        ).astype(jnp.float32).astype(jnp.bfloat16)
        high, middle, low = split3(shifted)
        total = (dot32(low, sibling) + dot32(middle, sibling)) + dot32(high, sibling)
        parent_out[...] = total[:NCOEF]

    return (
        lambda: (begin(), sums_of((0,))),
        lambda: sums_of((1, 2)),
        lambda: sums_of(tuple(range(3, ORDER + 1))),
        parents,
    )


def store_all(final, leaf_final, leaf_in, parent_in, positions, charges, velocities, leaves,
              leaf_out, parent_out, sem):
    pairs = (
        (final.at[0:3], positions),
        (final.at[3], charges),
        (final.at[4:7], velocities),
        (leaf_final.at[0:1], leaves),
        (leaf_in, leaf_out),
        (parent_in, parent_out),
    )
    copies = [pltpu.make_async_copy(*pair, sem.at[k]) for k, pair in enumerate(pairs)]
    for copy in copies:
        copy.start()
    for copy in copies:
        copy.wait()


def per_device(positions, charges, velocities, leaf_ids, live_counts, send_counts):
    vmem = pl.BlockSpec(memory_space=pltpu.VMEM)
    smem = pl.BlockSpec(memory_space=pltpu.SMEM)
    anywhere = pl.BlockSpec(memory_space=pl.ANY)
    f32 = jnp.float32
    copies = len(FRAMES) * len(CHUNKS)
    square = pltpu.VMEM((CAP, 128), f32)
    operands = (
        live_counts,
        send_counts,
        leaf_ids.reshape(1, CAP),
        positions,
        charges,
        velocities,
        shift_table(),
    )
    results = pl.pallas_call(
        exchange,
        name="exchange",
        out_shape=(
            jax.ShapeDtypeStruct((COMPS, CAP, 128), f32),
            jax.ShapeDtypeStruct((8, CAP), jnp.int32),
            jax.ShapeDtypeStruct((NCOEF, CAP), f32),
            jax.ShapeDtypeStruct((NCOEF, CAP), f32),
        ),
        in_specs=[anywhere] * 7,
        out_specs=(vmem,) * 4,
        scratch_shapes=[
            pltpu.SMEM((256,), jnp.int32),
            pltpu.SMEM((8, 256), jnp.int32),
            pltpu.VMEM((1, CAP), jnp.int32),
            pltpu.VMEM((COMPS, LIST_BASE + CAP + 64, 128), f32),
            pltpu.VMEM((COMPS, LIST_BASE + CAP + 64, 128), f32),
            pltpu.VMEM((COMPS, FP_BASE + CAP + 64, 128), f32),
            pltpu.VMEM((COMPS, FR_BASE + 2 * SLAB, 128), f32),
            pltpu.VMEM((COMPS, X_BASE + CAP, 128), f32),
            pltpu.VMEM((2 * len(PHASES), FRAME, 128), f32),
            pltpu.VMEM((3 * len(PHASES), FRAME, 128), f32),
            pltpu.VMEM((ROWS, ROWS), jnp.bfloat16),
        ]
        + [square] * 5
        + [
            pltpu.VMEM((ROWS, 128), f32),
            pltpu.VMEM((ROWS, 128), f32),
            pltpu.SemaphoreType.DMA((4 + COMPS,)),
            pltpu.SemaphoreType.DMA((copies,)),
            pltpu.SemaphoreType.DMA((copies,)),
            pltpu.SemaphoreType.REGULAR,
        ],
        compiler_params=pltpu.CompilerParams(
            collective_id=0, has_side_effects=True, vmem_limit_bytes=VMEM_LIMIT
        ),
    )(*(pltpu.with_memory_space_constraint(operand, pltpu.HBM) for operand in operands))

    outs = pl.pallas_call(
        store_all,
        name="store_all",
        out_shape=(
            jax.ShapeDtypeStruct((3, CAP, 128), f32),
            jax.ShapeDtypeStruct((CAP, 128), f32),
            jax.ShapeDtypeStruct((3, CAP, 128), f32),
            jax.ShapeDtypeStruct((1, CAP), jnp.int32),
            jax.ShapeDtypeStruct((NCOEF, CAP), f32),
            jax.ShapeDtypeStruct((NCOEF, CAP), f32),
        ),
        in_specs=[vmem] * 4,
        out_specs=(anywhere,) * 6,
        scratch_shapes=[pltpu.SemaphoreType.DMA((6,))],
        compiler_params=pltpu.CompilerParams(vmem_limit_bytes=4 * 2**20),
    )(*results)
    moved_positions, moved_charges, moved_velocities, moved_leaves, leaf_part, parent_part = outs
    return (
        moved_positions,
        moved_charges,
        moved_velocities,
        moved_leaves.reshape(CAP),
        leaf_part,
        parent_part,
    )


def solution(mesh):
    names = ("gx", "gy", "gz")
    in_specs = (P(None, names, None), P(names, None), P(None, names, None), P(names), P(), P())
    out_specs = (
        P(None, names, None),
        P(names, None),
        P(None, names, None),
        P(names),
        P(None, names),
        P(None, names),
    )
    return jax.shard_map(
        per_device, mesh=mesh, in_specs=in_specs, out_specs=out_specs, check_vma=False
    )
```

```python
import functools
import math

import jax
import jax.numpy as jnp
import numpy as np
from jax import lax
from jax.experimental import pallas as pl
from jax.experimental.pallas import tpu as pltpu
from jax.sharding import PartitionSpec as P

ORDER = 10
LEVEL = 7
CAP = 128
SLAB = 32
COMPS = 7
FRAME = SLAB * COMPS + 8
LEAF_ROWS = slice(SLAB * 4, SLAB * 4 + 8)
CHUNKS = ((0, 1), (1, 2), (2, 4), (4, 6), (6, 7))
MESH = pl.DeviceIdType.MESH

PHASES = (
('gx', (2, 1), 0),
('gy', (4, 2), 2),
('gy', (1,), 4),
('gz', (4, 2), 5),
('gz', (1,), 7),
)
SIZES = {"gx": 4, "gy": 8, "gz": 8}
STRIDES = {"gx": 64, "gy": 8, "gz": 1}
FRAMES = [(p, slot) for p, phase in enumerate(PHASES) for slot in range(2 ** len(phase[1]) - 1)]
VMEM_LIMIT = 24 * 2**20
ORDER_OF_WORK = [(-1, 0), (-1, 1), (-1, 2), (-1, 3), (-1, 4), (0, 0), (0, 1), (0, 2), (1, 0), (0, 3), (1, 1), (2, 0), (0, 4), (2, 1), (1, 2), (2, 2), (1, 3), (1, 4), (2, 3), (3, 0), (2, 4), (3, 1), (3, 2), (4, 0), (3, 3), (4, 1), (4, 2), 0, (3, 4), 1, 2, 3, (4, 3), (4, 4)]
LIST_BASE = 64
FP_BASE = 160
X_BASE = 128
FR_BASE = 32

TRIPLES = [
    (p, q, r)
    for p in range(ORDER + 1)
    for q in range(ORDER + 1 - p)
    for r in range(ORDER + 1 - p - q)
]
NCOEF = len(TRIPLES)
ROWS = 288


def bits_of(value):
    high = jnp.where(value >= 4, 1, 0)
    rest = value - 4 * high
    middle = jnp.where(rest >= 2, 1, 0)
    return {4: high, 2: middle, 1: rest - 2 * middle}


def rows_of(first, end):
    return slice(SLAB * first + 8 * (first >= 4), SLAB * end + 8 * (end >= 4))


def frame_rows(k):
    start = SLAB * k + 8 * (k >= 4)
    return slice(start, start + SLAB)


def pick(bit, one, zero):
    return bit * one + (1 - bit) * zero


def exchange(live_hbm, sends_hbm, leaves_hbm, positions, charges, velocities, table_hbm,
             final, leaf_final, leaf_out, parent_out,
             live, sends, leaves, list_a, list_b, frame_p, frame_r, frame_x, out, land,
             table, u_ref, v_ref, w_ref, a_ref, b_ref, flip_ref, sign_ref,
             load_sem, send_sem, recv_sem, vouched):
    moment_refs = (leaf_out, parent_out, u_ref, v_ref, w_ref, a_ref, b_ref, flip_ref, sign_ref)
    where = {axis: lax.axis_index(axis) for axis in SIZES}
    bits = {axis: bits_of(where[axis]) for axis in SIZES}
    me = sum(where[axis] * STRIDES[axis] for axis in SIZES)

    def step_of(axis, mask):
        return sum(m - 2 * m * bits[axis][m] for m in (4, 2, 1) if mask & m)

    def peer(axis, mask):
        return {axis: where[axis] + step_of(axis, mask)}

    def device(flips):
        return me + sum(step_of(axis, mask) * STRIDES[axis] for axis, mask in flips)

    def moved(flips, axis, mask):
        return flips ^ {(axis, mask)}

    barrier = pltpu.get_barrier_semaphore()
    partners = 0
    for axis, masks, _ in PHASES:
        for mask in masks + ((sum(masks),) if len(masks) == 2 else ()):
            if (axis, mask) == ("gz", 4):
                continue
            pl.semaphore_signal(
                barrier, inc=1, device_id=peer(axis, mask), device_id_type=MESH
            )
            partners += 1
    lists = (list_a, list_b)
    body = slice(LIST_BASE, LIST_BASE + CAP)
    pairs = [(live_hbm, live), (sends_hbm, sends), (leaves_hbm, leaves)]
    pairs += [(positions.at[k], list_a.at[k, body]) for k in range(3)]
    pairs += [(charges, list_a.at[3, body])]
    pairs += [(velocities.at[k], list_a.at[4 + k, body]) for k in range(3)]
    pairs += [(table_hbm, table)]
    loads = [
        pltpu.make_async_copy(source, target, load_sem.at[k])
        for k, (source, target) in enumerate(pairs)
    ]
    for load in loads:
        load.start()
    for load in loads[:2]:
        load.wait()

    def section_step(coords, count, section, axis, mask):
        sent = sends[section, device(coords)]
        got = sends[section, device(moved(coords, axis, mask))]
        return sent, got, count - sent + got

    def start_count(coords, phase_now):
        count = live[device(coords)]
        for axis, masks, section in PHASES[:phase_now]:
            for step, mask in enumerate(masks):
                count = section_step(coords, count, section + step, axis, mask)[2]
        return count

    plans = []
    here = frozenset()
    count = live[device(here)]
    for phase_now, (axis, masks, section) in enumerate(PHASES):
        plan = {}
        m1 = masks[0]
        a = bits[axis][m1]
        sent, got, count1 = section_step(here, count, section, axis, m1)
        kept = count - sent
        plan["start_a"] = pick(a, 0, kept)
        fs = pick(a, 0, kept)
        dl = pick(a, sent - got, 0)
        if len(masks) == 2:
            m2 = masks[1]
            b = bits[axis][m2]
            sent1, got1, count2 = section_step(here, count1, section + 1, axis, m2)
            kept1 = count1 - sent1
            start_b = pick(b, 0, kept1)
            plan["start_q"] = start_b + dl
            d1 = pick(b, sent1 - got1, 0)
            xs = pick(b, 0, kept1)
            plan["fs"] = fs - d1
            plan["list_off"] = dl + d1
            plan["xs"] = xs
            plan["xe"] = xs + got1
            other = moved(here, axis, m2)
            count_q = start_count(other, phase_now)
            sent_q, got_q, count1_q = section_step(other, count_q, section, axis, m1)
            fs_q = pick(a, 0, count_q - sent_q)
            start_bq = pick(b, count1_q - got1, 0)
            off_r = start_bq - fs_q
            plan["off_r"] = jnp.maximum(jnp.minimum(off_r, SLAB), -SLAB)
            plan["got_q"] = got_q
            count = count2
        else:
            plan["fs"] = fs
            plan["list_off"] = dl
            count = count1
        plan["fe"] = plan["fs"] + got
        plan["count"] = count
        plans.append(plan)

    def transfers(p, j):
        axis, masks, _ = PHASES[p]
        first, end = CHUNKS[j]
        rows = rows_of(first, end)
        todo = [(0, 0, masks[0])]
        if len(masks) == 2:
            todo += [(1, 1, masks[1]), (2, 0, masks[0] + masks[1])]
        copies = []
        for slot, source, mask in todo:
            at = FRAMES.index((p, slot)) * len(CHUNKS) + j
            copies.append(
                pltpu.make_async_remote_copy(
                    src_ref=out.at[2 * p + source, rows],
                    dst_ref=land.at[3 * p + slot, rows],
                    send_sem=send_sem.at[at],
                    recv_sem=recv_sem.at[at],
                    device_id=peer(axis, mask),
                    device_id_type=MESH,
                )
            )
        return copies

    started = {}
    leaf_list = {}

    def to_left(row, amount):
        return pltpu.roll(row, (4 * 128 - amount) % 128, 1)

    def send(p, j):
        now, plan = lists[p % 2], plans[p]
        first, end = CHUNKS[j]
        two = "start_q" in plan
        for k in range(first, end):
            rows = frame_rows(k)
            out[2 * p, rows] = now[k, pl.ds(LIST_BASE + plan["start_a"], SLAB), :]
            if two:
                out[2 * p + 1, rows] = now[k, pl.ds(LIST_BASE + plan["start_q"], SLAB), :]
        if end == 4:
            out[2 * p, LEAF_ROWS] = to_left(leaf_list[p], plan["start_a"])
            if two:
                out[2 * p + 1, LEAF_ROWS] = to_left(leaf_list[p], plan["start_q"])
        started[p, j] = transfers(p, j)
        for copy in started[p, j]:
            copy.start()

    def receive(p, j):
        now, plan = lists[p % 2], plans[p]
        last = p == len(PHASES) - 1
        first, end = CHUNKS[j]
        for copy in started[p, j]:
            copy.wait_recv()
        two = "start_q" in plan
        for k in range(first, end):
            rows = frame_rows(k)
            frame_p[k, FP_BASE : FP_BASE + SLAB] = land[3 * p, rows]
            if two:
                frame_r[k, FR_BASE : FR_BASE + SLAB] = land[3 * p + 2, rows]
        if two:
            row = lax.broadcasted_iota(jnp.int32, (SLAB, 128), 0) + plan["off_r"]
            from_r = (row >= 0) & (row < plan["got_q"])
            for k in range(first, end):
                frame_x[k, X_BASE : X_BASE + SLAB] = jnp.where(
                    from_r,
                    frame_r[k, pl.ds(FR_BASE + plan["off_r"], SLAB), :],
                    land[3 * p + 1, frame_rows(k)],
                )

        def tile(t, carry):
            base = t * 8
            row = lax.broadcasted_iota(jnp.int32, (8, 128), 0) + base
            from_p = (row >= plan["fs"]) & (row < plan["fe"])
            if two:
                from_x = (row >= plan["xs"]) & (row < plan["xe"])
            if last:
                full = row < plan["count"]
            for k in range(first, end):
                value = jnp.where(
                    from_p,
                    frame_p[k, pl.ds(FP_BASE - plan["fs"] + base, 8), :],
                    now[k, pl.ds(LIST_BASE + plan["list_off"] + base, 8), :],
                )
                if two:
                    value = jnp.where(
                        from_x, frame_x[k, pl.ds(X_BASE - plan["xs"] + base, 8), :], value
                    )
                if last:
                    final[k, pl.ds(base, 8), :] = jnp.where(full, value, 0.0)
                else:
                    lists[(p + 1) % 2][k, pl.ds(LIST_BASE + base, 8), :] = value
            return carry

        lax.fori_loop(0, CAP // 8, tile, 0, unroll=True)
        if end == 4:
            lane = lax.broadcasted_iota(jnp.int32, (8, 128), 1)
            value = jnp.where(
                (lane >= plan["fs"]) & (lane < plan["fe"]),
                to_left(land[3 * p, LEAF_ROWS], -plan["fs"]),
                to_left(leaf_list[p], plan["list_off"]),
            )
            if two:
                at = lane + plan["off_r"]
                second = jnp.where(
                    (at >= 0) & (at < plan["got_q"]),
                    to_left(land[3 * p + 2, LEAF_ROWS], plan["off_r"]),
                    land[3 * p + 1, LEAF_ROWS],
                )
                value = jnp.where(
                    (lane >= plan["xs"]) & (lane < plan["xe"]), to_left(second, -plan["xs"]), value
                )
            if last:
                leaf_final[...] = jnp.where(lane < plan["count"], value, -1.0).astype(jnp.int32)
            else:
                leaf_list[p + 1] = value

    for load in loads[2:]:
        load.wait()
    leaf_list[0] = jnp.broadcast_to(leaves[...], (8, 128)).astype(jnp.float32)
    pl.semaphore_wait(barrier, partners)
    pl.semaphore_signal(vouched, inc=1, device_id=peer("gz", 6), device_id_type=MESH)
    moments = moment_pieces(final, leaf_final, table, *moment_refs)
    for work in ORDER_OF_WORK:
        if isinstance(work, int):
            moments[work]()
            continue
        p, j = work
        if p >= 0:
            receive(p, j)
        if p + 1 < len(PHASES):
            if (p + 1, j) == (3, 0):
                pl.semaphore_wait(vouched, 1)
            send(p + 1, j)
    for copies in started.values():
        for copy in copies:
            copy.wait_send()


def shift_table():
    table = np.zeros((ROWS, ROWS), np.float32)
    for k, (p, q, r) in enumerate(TRIPLES):
        for j, (e, f, g) in enumerate(TRIPLES):
            if e <= p and f <= q and g <= r:
                table[k, j] = (
                    math.comb(p, e) * math.comb(q, f) * math.comb(r, g) * 0.5 ** (p + q + r)
                )
    return jnp.asarray(table, jnp.bfloat16)


def split3(value):
    high = value.astype(jnp.bfloat16)
    rest = value - high.astype(jnp.float32)
    middle = rest.astype(jnp.bfloat16)
    low = (rest - middle.astype(jnp.float32)).astype(jnp.bfloat16)
    return high, middle, low


def dot32(left, right):
    return jnp.dot(left, right, preferred_element_type=jnp.float32)


def packed_sums(parts):
    row = lax.broadcasted_iota(jnp.int32, (8, 128), 0)
    low = row < 4
    parts = [
        jnp.where(low, one, two) + pltpu.roll(jnp.where(low, two, one), 4, 0)
        for one, two in zip(parts[:4], parts[4:])
    ]
    for half in (2, 1):
        low = row % (2 * half) < half
        parts = [
            jnp.where(low, one, two)
            + jnp.where(low, pltpu.roll(one, 8 - half, 0), pltpu.roll(two, half, 0))
            for one, two in zip(parts[:half], parts[half:])
        ]
    return parts[0]


def moment_pieces(final, leaf_final, table, leaf_out, parent_out,
                  u_ref, v_ref, w_ref, a_ref, b_ref, flip_ref, sign_ref):
    state = {"sums": [], "k": 0}
    step = 16

    def begin():
        leaf_row = leaf_final[...]
        leaf = jnp.where(leaf_row >= 0, leaf_row, 0)
        cells = []
        for axis_bit in (2, 1, 0):
            cell = jnp.zeros_like(leaf)
            for level in range(LEVEL):
                cell = cell + ((leaf >> (3 * level + axis_bit)) & 1) * 2**level
            cells.append(cell[0:1].astype(jnp.float32))
        for axis, ref in enumerate((u_ref, v_ref, w_ref)):
            ref[...] = 2.0 * (final[axis].T * float(2**LEVEL) - cells[axis]) - 1.0
        a_ref[...] = final[3].T * (1.0 / 16.0)
        state["flips"] = [
            jnp.where(((leaf >> bit) & 1) == 1, 1.0, -1.0).astype(jnp.float32) for bit in (2, 1, 0)
        ]

    def store(parts, first):
        parts = parts + [jnp.zeros((8, 128), jnp.float32)] * (8 - len(parts))
        rows = packed_sums(parts)
        row = lax.broadcasted_iota(jnp.int32, (8, 128), 0)
        sign = jnp.ones((8, 128), jnp.float32)
        for axis in range(3):
            odd = sum(
                (TRIPLES[first + i][axis] & 1) << i for i in range(8) if first + i < NCOEF
            )
            if odd:
                sign = sign * jnp.where((odd >> row) & 1 == 1, state["flips"][axis], 1.0)
        count = min(8, NCOEF - first)
        leaf_out[first : first + count] = rows[:count]
        flip_ref[first : first + 8] = rows * sign
        sign_ref[first : first + 8] = sign

    def sums_of(orders):
        for p in orders:
            for q in range(ORDER + 1 - p):
                count = ORDER + 1 - p - q

                def body(g, sums, first=q == 0, more_q=q < ORDER - p, more_p=p < ORDER, count=count):
                    sums = list(sums)
                    for i in range(step):
                        rows = pl.ds((g * step + i) * 8, 8)
                        term = (a_ref if first else b_ref)[rows, :]
                        if more_q:
                            b_ref[rows, :] = term * v_ref[rows, :]
                        if first and more_p:
                            a_ref[rows, :] = term * u_ref[rows, :]
                        w = w_ref[rows, :]
                        for r in range(count):
                            sums[r] = sums[r] + term
                            if r + 1 < count:
                                term = term * w
                    return tuple(sums)

                zero = jnp.zeros((8, 128), jnp.float32)
                state["sums"] += list(lax.fori_loop(0, 16 // step, body, (zero,) * count))
                while len(state["sums"]) >= 8:
                    store(state["sums"][:8], state["k"])
                    state["sums"] = state["sums"][8:]
                    state["k"] += 8
        if orders[-1] == ORDER:
            store(state["sums"], state["k"])

    def parents():
        high, middle, low = split3(flip_ref[...])
        matrix = table[...]
        shifted = (dot32(matrix, low) + dot32(matrix, middle)) + dot32(matrix, high)
        shifted = shifted * sign_ref[...]
        leaf_row = leaf_final[0:1]
        leaf_col = (
            jnp.broadcast_to(leaf_row.astype(jnp.float32), (CAP, 128)).T.astype(jnp.int32)
        )
        sibling = (
            ((leaf_col >> 3) == (leaf_row >> 3)) & (leaf_col >= 0) & (leaf_row >= 0)
        ).astype(jnp.float32).astype(jnp.bfloat16)
        high, middle, low = split3(shifted)
        total = (dot32(low, sibling) + dot32(middle, sibling)) + dot32(high, sibling)
        parent_out[...] = total[:NCOEF]

    return (
        lambda: (begin(), sums_of((0,))),
        lambda: sums_of((1, 2)),
        lambda: sums_of(tuple(range(3, ORDER + 1))),
        parents,
    )


def store_all(final, leaf_final, leaf_in, parent_in, positions, charges, velocities, leaves,
              leaf_out, parent_out, sem):
    pairs = (
        (final.at[0:3], positions),
        (final.at[3], charges),
        (final.at[4:7], velocities),
        (leaf_final.at[0:1], leaves),
        (leaf_in, leaf_out),
        (parent_in, parent_out),
    )
    copies = [pltpu.make_async_copy(*pair, sem.at[k]) for k, pair in enumerate(pairs)]
    for copy in copies:
        copy.start()
    for copy in copies:
        copy.wait()


def per_device(positions, charges, velocities, leaf_ids, live_counts, send_counts):
    vmem = pl.BlockSpec(memory_space=pltpu.VMEM)
    smem = pl.BlockSpec(memory_space=pltpu.SMEM)
    anywhere = pl.BlockSpec(memory_space=pl.ANY)
    f32 = jnp.float32
    copies = len(FRAMES) * len(CHUNKS)
    square = pltpu.VMEM((CAP, 128), f32)
    operands = (
        live_counts,
        send_counts,
        leaf_ids.reshape(1, CAP),
        positions,
        charges,
        velocities,
        shift_table(),
    )
    results = pl.pallas_call(
        exchange,
        name="exchange",
        out_shape=(
            jax.ShapeDtypeStruct((COMPS, CAP, 128), f32),
            jax.ShapeDtypeStruct((8, CAP), jnp.int32),
            jax.ShapeDtypeStruct((NCOEF, CAP), f32),
            jax.ShapeDtypeStruct((NCOEF, CAP), f32),
        ),
        in_specs=[anywhere] * 7,
        out_specs=(vmem,) * 4,
        scratch_shapes=[
            pltpu.SMEM((256,), jnp.int32),
            pltpu.SMEM((8, 256), jnp.int32),
            pltpu.VMEM((1, CAP), jnp.int32),
            pltpu.VMEM((COMPS, LIST_BASE + CAP + 64, 128), f32),
            pltpu.VMEM((COMPS, LIST_BASE + CAP + 64, 128), f32),
            pltpu.VMEM((COMPS, FP_BASE + CAP + 64, 128), f32),
            pltpu.VMEM((COMPS, FR_BASE + 2 * SLAB, 128), f32),
            pltpu.VMEM((COMPS, X_BASE + CAP, 128), f32),
            pltpu.VMEM((2 * len(PHASES), FRAME, 128), f32),
            pltpu.VMEM((3 * len(PHASES), FRAME, 128), f32),
            pltpu.VMEM((ROWS, ROWS), jnp.bfloat16),
        ]
        + [square] * 5
        + [
            pltpu.VMEM((ROWS, 128), f32),
            pltpu.VMEM((ROWS, 128), f32),
            pltpu.SemaphoreType.DMA((4 + COMPS,)),
            pltpu.SemaphoreType.DMA((copies,)),
            pltpu.SemaphoreType.DMA((copies,)),
            pltpu.SemaphoreType.REGULAR,
        ],
        compiler_params=pltpu.CompilerParams(
            collective_id=0, has_side_effects=True, vmem_limit_bytes=VMEM_LIMIT
        ),
    )(*(pltpu.with_memory_space_constraint(operand, pltpu.HBM) for operand in operands))

    outs = pl.pallas_call(
        store_all,
        name="store_all",
        out_shape=(
            jax.ShapeDtypeStruct((3, CAP, 128), f32),
            jax.ShapeDtypeStruct((CAP, 128), f32),
            jax.ShapeDtypeStruct((3, CAP, 128), f32),
            jax.ShapeDtypeStruct((1, CAP), jnp.int32),
            jax.ShapeDtypeStruct((NCOEF, CAP), f32),
            jax.ShapeDtypeStruct((NCOEF, CAP), f32),
        ),
        in_specs=[vmem] * 4,
        out_specs=(anywhere,) * 6,
        scratch_shapes=[pltpu.SemaphoreType.DMA((6,))],
        compiler_params=pltpu.CompilerParams(vmem_limit_bytes=4 * 2**20),
    )(*results)
    moved_positions, moved_charges, moved_velocities, moved_leaves, leaf_part, parent_part = outs
    return (
        moved_positions,
        moved_charges,
        moved_velocities,
        moved_leaves.reshape(CAP),
        leaf_part,
        parent_part,
    )


def solution(mesh):
    names = ("gx", "gy", "gz")
    in_specs = (P(None, names, None), P(names, None), P(None, names, None), P(names), P(), P())
    out_specs = (
        P(None, names, None),
        P(names, None),
        P(None, names, None),
        P(names),
        P(None, names),
        P(None, names),
    )
    return jax.shard_map(
        per_device, mesh=mesh, in_specs=in_specs, out_specs=out_specs, check_vma=False
    )
```

```python
import functools
import math

import jax
import jax.numpy as jnp
import numpy as np
from jax import lax
from jax.experimental import pallas as pl
from jax.experimental.pallas import tpu as pltpu
from jax.sharding import PartitionSpec as P

ORDER = 10
LEVEL = 7
CAP = 128
SLAB = 32
COMPS = 7
FRAME = SLAB * COMPS + 8
LEAF_ROWS = slice(SLAB * 4, SLAB * 4 + 8)
CHUNKS = ((0, 1), (1, 2), (2, 4), (4, 6), (6, 7))
MESH = pl.DeviceIdType.MESH

PHASES = (
('gx', (2, 1), 0),
('gy', (4, 2), 2),
('gy', (1,), 4),
('gz', (4, 2), 5),
('gz', (1,), 7),
)
SIZES = {"gx": 4, "gy": 8, "gz": 8}
STRIDES = {"gx": 64, "gy": 8, "gz": 1}
FRAMES = [(p, slot) for p, phase in enumerate(PHASES) for slot in range(2 ** len(phase[1]) - 1)]
VMEM_LIMIT = 24 * 2**20
ORDER_OF_WORK = [(-1, 0), (-1, 1), (-1, 2), (-1, 3), (-1, 4), (0, 0), (0, 1), (0, 2), (1, 0), (0, 3), (1, 1), (2, 0), (0, 4), (2, 1), (1, 2), (2, 2), (1, 3), (1, 4), (2, 3), (3, 0), (2, 4), (3, 1), (3, 2), (4, 0), 5, (3, 3), (4, 1), 6, (3, 4), (4, 2), 0, 1, 2, (4, 3), 3, 4, (4, 4)]
LIST_BASE = 64
FP_BASE = 160
X_BASE = 128
FR_BASE = 32

TRIPLES = [
    (p, q, r)
    for p in range(ORDER + 1)
    for q in range(ORDER + 1 - p)
    for r in range(ORDER + 1 - p - q)
]
NCOEF = len(TRIPLES)
ROWS = 288


def bits_of(value):
    high = jnp.where(value >= 4, 1, 0)
    rest = value - 4 * high
    middle = jnp.where(rest >= 2, 1, 0)
    return {4: high, 2: middle, 1: rest - 2 * middle}


def rows_of(first, end):
    return slice(SLAB * first + 8 * (first >= 4), SLAB * end + 8 * (end >= 4))


def frame_rows(k):
    start = SLAB * k + 8 * (k >= 4)
    return slice(start, start + SLAB)


def pick(bit, one, zero):
    return bit * one + (1 - bit) * zero


def exchange(live_hbm, sends_hbm, leaves_hbm, positions, charges, velocities, table_hbm,
             final, leaf_final, leaf_out, parent_out,
             live, sends, leaves, list_a, list_b, frame_p, frame_r, frame_x, out, land,
             table, u_ref, v_ref, w_ref, a_ref, b_ref, flip_ref, sign_ref,
             load_sem, send_sem, recv_sem, vouched):
    moment_refs = (leaf_out, parent_out, u_ref, v_ref, w_ref, a_ref, b_ref, flip_ref, sign_ref)
    where = {axis: lax.axis_index(axis) for axis in SIZES}
    bits = {axis: bits_of(where[axis]) for axis in SIZES}
    me = sum(where[axis] * STRIDES[axis] for axis in SIZES)

    def step_of(axis, mask):
        return sum(m - 2 * m * bits[axis][m] for m in (4, 2, 1) if mask & m)

    def peer(axis, mask):
        return {axis: where[axis] + step_of(axis, mask)}

    def device(flips):
        return me + sum(step_of(axis, mask) * STRIDES[axis] for axis, mask in flips)

    def moved(flips, axis, mask):
        return flips ^ {(axis, mask)}

    barrier = pltpu.get_barrier_semaphore()
    partners = 0
    for axis, masks, _ in PHASES:
        for mask in masks + ((sum(masks),) if len(masks) == 2 else ()):
            if (axis, mask) == ("gz", 4):
                continue
            pl.semaphore_signal(
                barrier, inc=1, device_id=peer(axis, mask), device_id_type=MESH
            )
            partners += 1
    lists = (list_a, list_b)
    body = slice(LIST_BASE, LIST_BASE + CAP)
    pairs = [(live_hbm, live), (sends_hbm, sends), (leaves_hbm, leaves)]
    pairs += [(positions.at[k], list_a.at[k, body]) for k in range(3)]
    pairs += [(charges, list_a.at[3, body])]
    pairs += [(velocities.at[k], list_a.at[4 + k, body]) for k in range(3)]
    pairs += [(table_hbm, table)]
    loads = [
        pltpu.make_async_copy(source, target, load_sem.at[k])
        for k, (source, target) in enumerate(pairs)
    ]
    for load in loads:
        load.start()
    for load in loads[:2]:
        load.wait()

    def section_step(coords, count, section, axis, mask):
        sent = sends[section, device(coords)]
        got = sends[section, device(moved(coords, axis, mask))]
        return sent, got, count - sent + got

    def start_count(coords, phase_now):
        count = live[device(coords)]
        for axis, masks, section in PHASES[:phase_now]:
            for step, mask in enumerate(masks):
                count = section_step(coords, count, section + step, axis, mask)[2]
        return count

    plans = []
    here = frozenset()
    count = live[device(here)]
    for phase_now, (axis, masks, section) in enumerate(PHASES):
        plan = {}
        m1 = masks[0]
        a = bits[axis][m1]
        sent, got, count1 = section_step(here, count, section, axis, m1)
        kept = count - sent
        plan["start_a"] = pick(a, 0, kept)
        fs = pick(a, 0, kept)
        dl = pick(a, sent - got, 0)
        if len(masks) == 2:
            m2 = masks[1]
            b = bits[axis][m2]
            sent1, got1, count2 = section_step(here, count1, section + 1, axis, m2)
            kept1 = count1 - sent1
            start_b = pick(b, 0, kept1)
            plan["start_q"] = start_b + dl
            d1 = pick(b, sent1 - got1, 0)
            xs = pick(b, 0, kept1)
            plan["fs"] = fs - d1
            plan["list_off"] = dl + d1
            plan["xs"] = xs
            plan["xe"] = xs + got1
            other = moved(here, axis, m2)
            count_q = start_count(other, phase_now)
            sent_q, got_q, count1_q = section_step(other, count_q, section, axis, m1)
            fs_q = pick(a, 0, count_q - sent_q)
            start_bq = pick(b, count1_q - got1, 0)
            off_r = start_bq - fs_q
            plan["off_r"] = jnp.maximum(jnp.minimum(off_r, SLAB), -SLAB)
            plan["got_q"] = got_q
            count = count2
        else:
            plan["fs"] = fs
            plan["list_off"] = dl
            count = count1
        plan["fe"] = plan["fs"] + got
        plan["count"] = count
        plans.append(plan)

    def transfers(p, j):
        axis, masks, _ = PHASES[p]
        first, end = CHUNKS[j]
        rows = rows_of(first, end)
        todo = [(0, 0, masks[0])]
        if len(masks) == 2:
            todo += [(1, 1, masks[1]), (2, 0, masks[0] + masks[1])]
        copies = []
        for slot, source, mask in todo:
            at = FRAMES.index((p, slot)) * len(CHUNKS) + j
            copies.append(
                pltpu.make_async_remote_copy(
                    src_ref=out.at[2 * p + source, rows],
                    dst_ref=land.at[3 * p + slot, rows],
                    send_sem=send_sem.at[at],
                    recv_sem=recv_sem.at[at],
                    device_id=peer(axis, mask),
                    device_id_type=MESH,
                )
            )
        return copies

    started = {}
    leaf_list = {}

    def to_left(row, amount):
        return pltpu.roll(row, (4 * 128 - amount) % 128, 1)

    def send(p, j):
        now, plan = lists[p % 2], plans[p]
        first, end = CHUNKS[j]
        two = "start_q" in plan
        for k in range(first, end):
            rows = frame_rows(k)
            out[2 * p, rows] = now[k, pl.ds(LIST_BASE + plan["start_a"], SLAB), :]
            if two:
                out[2 * p + 1, rows] = now[k, pl.ds(LIST_BASE + plan["start_q"], SLAB), :]
        if end == 4:
            out[2 * p, LEAF_ROWS] = to_left(leaf_list[p], plan["start_a"])
            if two:
                out[2 * p + 1, LEAF_ROWS] = to_left(leaf_list[p], plan["start_q"])
        started[p, j] = transfers(p, j)
        for copy in started[p, j]:
            copy.start()

    def receive(p, j):
        now, plan = lists[p % 2], plans[p]
        last = p == len(PHASES) - 1
        first, end = CHUNKS[j]
        for copy in started[p, j]:
            copy.wait_recv()
        two = "start_q" in plan
        for k in range(first, end):
            rows = frame_rows(k)
            frame_p[k, FP_BASE : FP_BASE + SLAB] = land[3 * p, rows]
            if two:
                frame_r[k, FR_BASE : FR_BASE + SLAB] = land[3 * p + 2, rows]
        if two:
            row = lax.broadcasted_iota(jnp.int32, (SLAB, 128), 0) + plan["off_r"]
            from_r = (row >= 0) & (row < plan["got_q"])
            for k in range(first, end):
                frame_x[k, X_BASE : X_BASE + SLAB] = jnp.where(
                    from_r,
                    frame_r[k, pl.ds(FR_BASE + plan["off_r"], SLAB), :],
                    land[3 * p + 1, frame_rows(k)],
                )

        def tile(t, carry):
            base = t * 8
            row = lax.broadcasted_iota(jnp.int32, (8, 128), 0) + base
            from_p = (row >= plan["fs"]) & (row < plan["fe"])
            if two:
                from_x = (row >= plan["xs"]) & (row < plan["xe"])
            if last:
                full = row < plan["count"]
            for k in range(first, end):
                value = jnp.where(
                    from_p,
                    frame_p[k, pl.ds(FP_BASE - plan["fs"] + base, 8), :],
                    now[k, pl.ds(LIST_BASE + plan["list_off"] + base, 8), :],
                )
                if two:
                    value = jnp.where(
                        from_x, frame_x[k, pl.ds(X_BASE - plan["xs"] + base, 8), :], value
                    )
                if last:
                    final[k, pl.ds(base, 8), :] = jnp.where(full, value, 0.0)
                else:
                    lists[(p + 1) % 2][k, pl.ds(LIST_BASE + base, 8), :] = value
            return carry

        lax.fori_loop(0, CAP // 8, tile, 0, unroll=True)
        if end == 4:
            lane = lax.broadcasted_iota(jnp.int32, (8, 128), 1)
            value = jnp.where(
                (lane >= plan["fs"]) & (lane < plan["fe"]),
                to_left(land[3 * p, LEAF_ROWS], -plan["fs"]),
                to_left(leaf_list[p], plan["list_off"]),
            )
            if two:
                at = lane + plan["off_r"]
                second = jnp.where(
                    (at >= 0) & (at < plan["got_q"]),
                    to_left(land[3 * p + 2, LEAF_ROWS], plan["off_r"]),
                    land[3 * p + 1, LEAF_ROWS],
                )
                value = jnp.where(
                    (lane >= plan["xs"]) & (lane < plan["xe"]), to_left(second, -plan["xs"]), value
                )
            if last:
                leaf_final[...] = jnp.where(lane < plan["count"], value, -1.0).astype(jnp.int32)
            else:
                leaf_list[p + 1] = value

    for load in loads[2:]:
        load.wait()
    leaf_list[0] = jnp.broadcast_to(leaves[...], (8, 128)).astype(jnp.float32)
    pl.semaphore_wait(barrier, partners)
    pl.semaphore_signal(vouched, inc=1, device_id=peer("gz", 6), device_id_type=MESH)
    moments = moment_pieces(final, leaf_final, table, *moment_refs)
    for work in ORDER_OF_WORK:
        if isinstance(work, int):
            moments[work]()
            continue
        p, j = work
        if p >= 0:
            receive(p, j)
        if p + 1 < len(PHASES):
            if (p + 1, j) == (3, 0):
                pl.semaphore_wait(vouched, 1)
            send(p + 1, j)
    for copies in started.values():
        for copy in copies:
            copy.wait_send()


def shift_table():
    table = np.zeros((ROWS, ROWS), np.float32)
    for k, (p, q, r) in enumerate(TRIPLES):
        for j, (e, f, g) in enumerate(TRIPLES):
            if e <= p and f <= q and g <= r:
                table[k, j] = (
                    math.comb(p, e) * math.comb(q, f) * math.comb(r, g) * 0.5 ** (p + q + r)
                )
    return jnp.asarray(table, jnp.bfloat16)


def split3(value):
    high = value.astype(jnp.bfloat16)
    rest = value - high.astype(jnp.float32)
    middle = rest.astype(jnp.bfloat16)
    low = (rest - middle.astype(jnp.float32)).astype(jnp.bfloat16)
    return high, middle, low


def dot32(left, right):
    return jnp.dot(left, right, preferred_element_type=jnp.float32)


def packed_sums(parts):
    row = lax.broadcasted_iota(jnp.int32, (8, 128), 0)
    low = row < 4
    parts = [
        jnp.where(low, one, two) + pltpu.roll(jnp.where(low, two, one), 4, 0)
        for one, two in zip(parts[:4], parts[4:])
    ]
    for half in (2, 1):
        low = row % (2 * half) < half
        parts = [
            jnp.where(low, one, two)
            + jnp.where(low, pltpu.roll(one, 8 - half, 0), pltpu.roll(two, half, 0))
            for one, two in zip(parts[:half], parts[half:])
        ]
    return parts[0]


def moment_pieces(final, leaf_final, table, leaf_out, parent_out,
                  u_ref, v_ref, w_ref, a_ref, b_ref, flip_ref, sign_ref):
    state = {"sums": [], "k": 0}

    def turn_x():
        u_ref[...] = final[0].T

    def turn_y():
        v_ref[...] = final[1].T

    def begin():
        leaf_row = leaf_final[...]
        leaf = jnp.where(leaf_row >= 0, leaf_row, 0)
        cells = []
        for axis_bit in (2, 1, 0):
            cell = jnp.zeros_like(leaf)
            for level in range(LEVEL):
                cell = cell + ((leaf >> (3 * level + axis_bit)) & 1) * 2**level
            cells.append(cell[0:1].astype(jnp.float32))
        w_ref[...] = final[2].T
        a_ref[...] = final[3].T * (1.0 / 16.0)
        for axis, ref in enumerate((u_ref, v_ref, w_ref)):
            ref[...] = 2.0 * (ref[...] * float(2**LEVEL) - cells[axis]) - 1.0
        state["flips"] = [
            jnp.where(((leaf >> bit) & 1) == 1, 1.0, -1.0).astype(jnp.float32) for bit in (2, 1, 0)
        ]

    def store(parts, first):
        parts = parts + [jnp.zeros((8, 128), jnp.float32)] * (8 - len(parts))
        rows = packed_sums(parts)
        row = lax.broadcasted_iota(jnp.int32, (8, 128), 0)
        sign = jnp.ones((8, 128), jnp.float32)
        for axis in range(3):
            odd = sum(
                (TRIPLES[first + i][axis] & 1) << i for i in range(8) if first + i < NCOEF
            )
            if odd:
                sign = sign * jnp.where((odd >> row) & 1 == 1, state["flips"][axis], 1.0)
        count = min(8, NCOEF - first)
        leaf_out[first : first + count] = rows[:count]
        flip_ref[first : first + 8] = rows * sign
        sign_ref[first : first + 8] = sign

    def sums_of(orders):
        for p in orders:
            for q in range(ORDER + 1 - p):
                count = ORDER + 1 - p - q

                sums = [None] * count
                for g in range(16):
                    rows = slice(8 * g, 8 * g + 8)
                    term = (a_ref if q == 0 else b_ref)[rows, :]
                    if q < ORDER - p:
                        b_ref[rows, :] = term * v_ref[rows, :]
                    if q == 0 and p < ORDER:
                        a_ref[rows, :] = term * u_ref[rows, :]
                    w = w_ref[rows, :]
                    for r in range(count):
                        sums[r] = term if g == 0 else sums[r] + term
                        if r + 1 < count:
                            term = term * w
                state["sums"] += sums
                while len(state["sums"]) >= 8:
                    store(state["sums"][:8], state["k"])
                    state["sums"] = state["sums"][8:]
                    state["k"] += 8
        if orders[-1] == ORDER:
            store(state["sums"], state["k"])

    def parents():
        high, middle, low = split3(flip_ref[...])
        matrix = table[...]
        shifted = (dot32(matrix, low) + dot32(matrix, middle)) + dot32(matrix, high)
        shifted = shifted * sign_ref[...]
        leaf_row = leaf_final[0:1]
        leaf_col = (
            jnp.broadcast_to(leaf_row.astype(jnp.float32), (CAP, 128)).T.astype(jnp.int32)
        )
        sibling = (
            ((leaf_col >> 3) == (leaf_row >> 3)) & (leaf_col >= 0) & (leaf_row >= 0)
        ).astype(jnp.float32).astype(jnp.bfloat16)
        high, middle, low = split3(shifted)
        total = (dot32(low, sibling) + dot32(middle, sibling)) + dot32(high, sibling)
        parent_out[...] = total[:NCOEF]

    return (
        begin,
        lambda: sums_of((0,)),
        lambda: sums_of((1, 2)),
        lambda: sums_of(tuple(range(3, ORDER + 1))),
        parents,
        turn_x,
        turn_y,
    )


def store_all(final, leaf_final, leaf_in, parent_in, positions, charges, velocities, leaves,
              leaf_out, parent_out, sem):
    pairs = (
        (final.at[0:3], positions),
        (final.at[3], charges),
        (final.at[4:7], velocities),
        (leaf_final.at[0:1], leaves),
        (leaf_in, leaf_out),
        (parent_in, parent_out),
    )
    copies = [pltpu.make_async_copy(*pair, sem.at[k]) for k, pair in enumerate(pairs)]
    for copy in copies:
        copy.start()
    for copy in copies:
        copy.wait()


def per_device(positions, charges, velocities, leaf_ids, live_counts, send_counts):
    vmem = pl.BlockSpec(memory_space=pltpu.VMEM)
    smem = pl.BlockSpec(memory_space=pltpu.SMEM)
    anywhere = pl.BlockSpec(memory_space=pl.ANY)
    f32 = jnp.float32
    copies = len(FRAMES) * len(CHUNKS)
    square = pltpu.VMEM((CAP, 128), f32)
    operands = (
        live_counts,
        send_counts,
        leaf_ids.reshape(1, CAP),
        positions,
        charges,
        velocities,
        shift_table(),
    )
    results = pl.pallas_call(
        exchange,
        name="exchange",
        out_shape=(
            jax.ShapeDtypeStruct((COMPS, CAP, 128), f32),
            jax.ShapeDtypeStruct((8, CAP), jnp.int32),
            jax.ShapeDtypeStruct((NCOEF, CAP), f32),
            jax.ShapeDtypeStruct((NCOEF, CAP), f32),
        ),
        in_specs=[anywhere] * 7,
        out_specs=(vmem,) * 4,
        scratch_shapes=[
            pltpu.SMEM((256,), jnp.int32),
            pltpu.SMEM((8, 256), jnp.int32),
            pltpu.VMEM((1, CAP), jnp.int32),
            pltpu.VMEM((COMPS, LIST_BASE + CAP + 64, 128), f32),
            pltpu.VMEM((COMPS, LIST_BASE + CAP + 64, 128), f32),
            pltpu.VMEM((COMPS, FP_BASE + CAP + 64, 128), f32),
            pltpu.VMEM((COMPS, FR_BASE + 2 * SLAB, 128), f32),
            pltpu.VMEM((COMPS, X_BASE + CAP, 128), f32),
            pltpu.VMEM((2 * len(PHASES), FRAME, 128), f32),
            pltpu.VMEM((3 * len(PHASES), FRAME, 128), f32),
            pltpu.VMEM((ROWS, ROWS), jnp.bfloat16),
        ]
        + [square] * 5
        + [
            pltpu.VMEM((ROWS, 128), f32),
            pltpu.VMEM((ROWS, 128), f32),
            pltpu.SemaphoreType.DMA((4 + COMPS,)),
            pltpu.SemaphoreType.DMA((copies,)),
            pltpu.SemaphoreType.DMA((copies,)),
            pltpu.SemaphoreType.REGULAR,
        ],
        compiler_params=pltpu.CompilerParams(
            collective_id=0, has_side_effects=True, vmem_limit_bytes=VMEM_LIMIT
        ),
    )(*(pltpu.with_memory_space_constraint(operand, pltpu.HBM) for operand in operands))

    outs = pl.pallas_call(
        store_all,
        name="store_all",
        out_shape=(
            jax.ShapeDtypeStruct((3, CAP, 128), f32),
            jax.ShapeDtypeStruct((CAP, 128), f32),
            jax.ShapeDtypeStruct((3, CAP, 128), f32),
            jax.ShapeDtypeStruct((1, CAP), jnp.int32),
            jax.ShapeDtypeStruct((NCOEF, CAP), f32),
            jax.ShapeDtypeStruct((NCOEF, CAP), f32),
        ),
        in_specs=[vmem] * 4,
        out_specs=(anywhere,) * 6,
        scratch_shapes=[pltpu.SemaphoreType.DMA((6,))],
        compiler_params=pltpu.CompilerParams(vmem_limit_bytes=4 * 2**20),
    )(*results)
    moved_positions, moved_charges, moved_velocities, moved_leaves, leaf_part, parent_part = outs
    return (
        moved_positions,
        moved_charges,
        moved_velocities,
        moved_leaves.reshape(CAP),
        leaf_part,
        parent_part,
    )


def solution(mesh):
    names = ("gx", "gy", "gz")
    in_specs = (P(None, names, None), P(names, None), P(None, names, None), P(names), P(), P())
    out_specs = (
        P(None, names, None),
        P(names, None),
        P(None, names, None),
        P(names),
        P(None, names),
        P(None, names),
    )
    return jax.shard_map(
        per_device, mesh=mesh, in_specs=in_specs, out_specs=out_specs, check_vma=False
    )
```

```python
import functools
import math

import jax
import jax.numpy as jnp
import numpy as np
from jax import lax
from jax.experimental import pallas as pl
from jax.experimental.pallas import tpu as pltpu
from jax.sharding import PartitionSpec as P

ORDER = 10
LEVEL = 7
CAP = 128
SLAB = 32
COMPS = 7
FRAME = SLAB * COMPS + 8
LEAF_ROWS = slice(SLAB * 4, SLAB * 4 + 8)
CHUNKS = ((0, 1), (1, 2), (2, 4), (4, 6), (6, 7))
MESH = pl.DeviceIdType.MESH

PHASES = (
('gx', (2, 1), 0),
('gy', (4, 2), 2),
('gy', (1,), 4),
('gz', (4, 2), 5),
('gz', (1,), 7),
)
SIZES = {"gx": 4, "gy": 8, "gz": 8}
STRIDES = {"gx": 64, "gy": 8, "gz": 1}
FRAMES = [(p, slot) for p, phase in enumerate(PHASES) for slot in range(2 ** len(phase[1]) - 1)]
VMEM_LIMIT = 24 * 2**20
ORDER_OF_WORK = [(-1, 0), (-1, 1), (-1, 2), (-1, 3), (-1, 4), (0, 0), (0, 1), (0, 2), (1, 0), (0, 3), (1, 1), (2, 0), (0, 4), (2, 1), (1, 2), (2, 2), (1, 3), (1, 4), (2, 3), (3, 0), (2, 4), (3, 1), (3, 2), (3, 3), (4, 0), 5, (4, 1), 6, (3, 4), (4, 2), 0, 1, 2, (4, 3), 3, 4, (4, 4)]
LIST_BASE = 64
FP_BASE = 160
X_BASE = 128
FR_BASE = 32

TRIPLES = [
    (p, q, r)
    for p in range(ORDER + 1)
    for q in range(ORDER + 1 - p)
    for r in range(ORDER + 1 - p - q)
]
NCOEF = len(TRIPLES)
ROWS = 288


def bits_of(value):
    high = jnp.where(value >= 4, 1, 0)
    rest = value - 4 * high
    middle = jnp.where(rest >= 2, 1, 0)
    return {4: high, 2: middle, 1: rest - 2 * middle}


def rows_of(first, end):
    return slice(SLAB * first + 8 * (first >= 4), SLAB * end + 8 * (end >= 4))


def frame_rows(k):
    start = SLAB * k + 8 * (k >= 4)
    return slice(start, start + SLAB)


def pick(bit, one, zero):
    return bit * one + (1 - bit) * zero


def exchange(live_hbm, sends_hbm, leaves_hbm, positions, charges, velocities, table_hbm,
             final, leaf_final, leaf_out, parent_out,
             live, sends, leaves, list_a, list_b, frame_p, frame_r, frame_x, out, land,
             table, u_ref, v_ref, w_ref, a_ref, b_ref, flip_ref, sign_ref,
             load_sem, send_sem, recv_sem, vouched):
    moment_refs = (leaf_out, parent_out, u_ref, v_ref, w_ref, a_ref, b_ref, flip_ref, sign_ref)
    where = {axis: lax.axis_index(axis) for axis in SIZES}
    bits = {axis: bits_of(where[axis]) for axis in SIZES}
    me = sum(where[axis] * STRIDES[axis] for axis in SIZES)

    def step_of(axis, mask):
        return sum(m - 2 * m * bits[axis][m] for m in (4, 2, 1) if mask & m)

    def peer(axis, mask):
        return {axis: where[axis] + step_of(axis, mask)}

    def device(flips):
        return me + sum(step_of(axis, mask) * STRIDES[axis] for axis, mask in flips)

    def moved(flips, axis, mask):
        return flips ^ {(axis, mask)}

    barrier = pltpu.get_barrier_semaphore()
    partners = 0
    for axis, masks, _ in PHASES:
        for mask in masks + ((sum(masks),) if len(masks) == 2 else ()):
            if (axis, mask) == ("gz", 4):
                continue
            pl.semaphore_signal(
                barrier, inc=1, device_id=peer(axis, mask), device_id_type=MESH
            )
            partners += 1
    lists = (list_a, list_b)
    body = slice(LIST_BASE, LIST_BASE + CAP)
    pairs = [(live_hbm, live), (sends_hbm, sends), (leaves_hbm, leaves)]
    pairs += [(positions.at[k], list_a.at[k, body]) for k in range(3)]
    pairs += [(charges, list_a.at[3, body])]
    pairs += [(velocities.at[k], list_a.at[4 + k, body]) for k in range(3)]
    pairs += [(table_hbm, table)]
    loads = [
        pltpu.make_async_copy(source, target, load_sem.at[k])
        for k, (source, target) in enumerate(pairs)
    ]
    for load in loads:
        load.start()
    for load in loads[:2]:
        load.wait()

    def section_step(coords, count, section, axis, mask):
        sent = sends[section, device(coords)]
        got = sends[section, device(moved(coords, axis, mask))]
        return sent, got, count - sent + got

    def start_count(coords, phase_now):
        count = live[device(coords)]
        for axis, masks, section in PHASES[:phase_now]:
            for step, mask in enumerate(masks):
                count = section_step(coords, count, section + step, axis, mask)[2]
        return count

    plans = []
    here = frozenset()
    count = live[device(here)]
    for phase_now, (axis, masks, section) in enumerate(PHASES):
        plan = {}
        m1 = masks[0]
        a = bits[axis][m1]
        sent, got, count1 = section_step(here, count, section, axis, m1)
        kept = count - sent
        plan["start_a"] = pick(a, 0, kept)
        fs = pick(a, 0, kept)
        dl = pick(a, sent - got, 0)
        if len(masks) == 2:
            m2 = masks[1]
            b = bits[axis][m2]
            sent1, got1, count2 = section_step(here, count1, section + 1, axis, m2)
            kept1 = count1 - sent1
            start_b = pick(b, 0, kept1)
            plan["start_q"] = start_b + dl
            d1 = pick(b, sent1 - got1, 0)
            xs = pick(b, 0, kept1)
            plan["fs"] = fs - d1
            plan["list_off"] = dl + d1
            plan["xs"] = xs
            plan["xe"] = xs + got1
            other = moved(here, axis, m2)
            count_q = start_count(other, phase_now)
            sent_q, got_q, count1_q = section_step(other, count_q, section, axis, m1)
            fs_q = pick(a, 0, count_q - sent_q)
            start_bq = pick(b, count1_q - got1, 0)
            off_r = start_bq - fs_q
            plan["off_r"] = jnp.maximum(jnp.minimum(off_r, SLAB), -SLAB)
            plan["got_q"] = got_q
            count = count2
        else:
            plan["fs"] = fs
            plan["list_off"] = dl
            count = count1
        plan["fe"] = plan["fs"] + got
        plan["count"] = count
        plans.append(plan)

    def transfers(p, j):
        axis, masks, _ = PHASES[p]
        first, end = CHUNKS[j]
        rows = rows_of(first, end)
        todo = [(0, 0, masks[0])]
        if len(masks) == 2:
            todo += [(2, 0, masks[0] + masks[1]), (1, 1, masks[1])]
        copies = []
        for slot, source, mask in todo:
            at = FRAMES.index((p, slot)) * len(CHUNKS) + j
            copies.append(
                pltpu.make_async_remote_copy(
                    src_ref=out.at[2 * p + source, rows],
                    dst_ref=land.at[3 * p + slot, rows],
                    send_sem=send_sem.at[at],
                    recv_sem=recv_sem.at[at],
                    device_id=peer(axis, mask),
                    device_id_type=MESH,
                )
            )
        return copies

    started = {}
    leaf_list = {}

    def to_left(row, amount):
        return pltpu.roll(row, (4 * 128 - amount) % 128, 1)

    def send(p, j):
        now, plan = lists[p % 2], plans[p]
        first, end = CHUNKS[j]
        two = "start_q" in plan
        for k in range(first, end):
            rows = frame_rows(k)
            out[2 * p, rows] = now[k, pl.ds(LIST_BASE + plan["start_a"], SLAB), :]
            if two:
                out[2 * p + 1, rows] = now[k, pl.ds(LIST_BASE + plan["start_q"], SLAB), :]
        if end == 4:
            out[2 * p, LEAF_ROWS] = to_left(leaf_list[p], plan["start_a"])
            if two:
                out[2 * p + 1, LEAF_ROWS] = to_left(leaf_list[p], plan["start_q"])
        started[p, j] = transfers(p, j)
        for copy in started[p, j]:
            copy.start()

    def receive(p, j):
        now, plan = lists[p % 2], plans[p]
        last = p == len(PHASES) - 1
        first, end = CHUNKS[j]
        for copy in started[p, j]:
            copy.wait_recv()
        two = "start_q" in plan
        for k in range(first, end):
            rows = frame_rows(k)
            frame_p[k, FP_BASE : FP_BASE + SLAB] = land[3 * p, rows]
            if two:
                frame_r[k, FR_BASE : FR_BASE + SLAB] = land[3 * p + 2, rows]
        if two:
            row = lax.broadcasted_iota(jnp.int32, (SLAB, 128), 0) + plan["off_r"]
            from_r = (row >= 0) & (row < plan["got_q"])
            for k in range(first, end):
                frame_x[k, X_BASE : X_BASE + SLAB] = jnp.where(
                    from_r,
                    frame_r[k, pl.ds(FR_BASE + plan["off_r"], SLAB), :],
                    land[3 * p + 1, frame_rows(k)],
                )

        def tile(t, carry):
            base = t * 8
            row = lax.broadcasted_iota(jnp.int32, (8, 128), 0) + base
            from_p = (row >= plan["fs"]) & (row < plan["fe"])
            if two:
                from_x = (row >= plan["xs"]) & (row < plan["xe"])
            if last:
                full = row < plan["count"]
            for k in range(first, end):
                value = jnp.where(
                    from_p,
                    frame_p[k, pl.ds(FP_BASE - plan["fs"] + base, 8), :],
                    now[k, pl.ds(LIST_BASE + plan["list_off"] + base, 8), :],
                )
                if two:
                    value = jnp.where(
                        from_x, frame_x[k, pl.ds(X_BASE - plan["xs"] + base, 8), :], value
                    )
                if last:
                    final[k, pl.ds(base, 8), :] = jnp.where(full, value, 0.0)
                else:
                    lists[(p + 1) % 2][k, pl.ds(LIST_BASE + base, 8), :] = value
            return carry

        lax.fori_loop(0, CAP // 8, tile, 0, unroll=True)
        if end == 4:
            lane = lax.broadcasted_iota(jnp.int32, (8, 128), 1)
            value = jnp.where(
                (lane >= plan["fs"]) & (lane < plan["fe"]),
                to_left(land[3 * p, LEAF_ROWS], -plan["fs"]),
                to_left(leaf_list[p], plan["list_off"]),
            )
            if two:
                at = lane + plan["off_r"]
                second = jnp.where(
                    (at >= 0) & (at < plan["got_q"]),
                    to_left(land[3 * p + 2, LEAF_ROWS], plan["off_r"]),
                    land[3 * p + 1, LEAF_ROWS],
                )
                value = jnp.where(
                    (lane >= plan["xs"]) & (lane < plan["xe"]), to_left(second, -plan["xs"]), value
                )
            if last:
                leaf_final[...] = jnp.where(lane < plan["count"], value, -1.0).astype(jnp.int32)
            else:
                leaf_list[p + 1] = value

    for load in loads[2:]:
        load.wait()
    leaf_list[0] = jnp.broadcast_to(leaves[...], (8, 128)).astype(jnp.float32)
    pl.semaphore_wait(barrier, partners)
    pl.semaphore_signal(vouched, inc=1, device_id=peer("gz", 6), device_id_type=MESH)
    moments = moment_pieces(final, leaf_final, table, *moment_refs)
    for work in ORDER_OF_WORK:
        if isinstance(work, int):
            moments[work]()
            continue
        p, j = work
        if p >= 0:
            receive(p, j)
        if p + 1 < len(PHASES):
            if (p + 1, j) == (3, 0):
                pl.semaphore_wait(vouched, 1)
            send(p + 1, j)
    for copies in started.values():
        for copy in copies:
            copy.wait_send()


def shift_table():
    table = np.zeros((ROWS, ROWS), np.float32)
    for k, (p, q, r) in enumerate(TRIPLES):
        for j, (e, f, g) in enumerate(TRIPLES):
            if e <= p and f <= q and g <= r:
                table[k, j] = (
                    math.comb(p, e) * math.comb(q, f) * math.comb(r, g) * 0.5 ** (p + q + r)
                )
    return jnp.asarray(table, jnp.bfloat16)


def split3(value):
    high = value.astype(jnp.bfloat16)
    rest = value - high.astype(jnp.float32)
    middle = rest.astype(jnp.bfloat16)
    low = (rest - middle.astype(jnp.float32)).astype(jnp.bfloat16)
    return high, middle, low


def dot32(left, right):
    return jnp.dot(left, right, preferred_element_type=jnp.float32)


def packed_sums(parts):
    row = lax.broadcasted_iota(jnp.int32, (8, 128), 0)
    low = row < 4
    parts = [
        jnp.where(low, one, two) + pltpu.roll(jnp.where(low, two, one), 4, 0)
        for one, two in zip(parts[:4], parts[4:])
    ]
    for half in (2, 1):
        low = row % (2 * half) < half
        parts = [
            jnp.where(low, one, two)
            + jnp.where(low, pltpu.roll(one, 8 - half, 0), pltpu.roll(two, half, 0))
            for one, two in zip(parts[:half], parts[half:])
        ]
    return parts[0]


def moment_pieces(final, leaf_final, table, leaf_out, parent_out,
                  u_ref, v_ref, w_ref, a_ref, b_ref, flip_ref, sign_ref):
    state = {"sums": [], "k": 0}

    def turn_x():
        u_ref[...] = final[0].T

    def turn_y():
        v_ref[...] = final[1].T

    def begin():
        leaf_row = leaf_final[...]
        leaf = jnp.where(leaf_row >= 0, leaf_row, 0)
        cells = []
        for axis_bit in (2, 1, 0):
            cell = jnp.zeros_like(leaf)
            for level in range(LEVEL):
                cell = cell + ((leaf >> (3 * level + axis_bit)) & 1) * 2**level
            cells.append(cell[0:1].astype(jnp.float32))
        w_ref[...] = final[2].T
        a_ref[...] = final[3].T * (1.0 / 16.0)
        for axis, ref in enumerate((u_ref, v_ref, w_ref)):
            ref[...] = 2.0 * (ref[...] * float(2**LEVEL) - cells[axis]) - 1.0
        state["flips"] = [
            jnp.where(((leaf >> bit) & 1) == 1, 1.0, -1.0).astype(jnp.float32) for bit in (2, 1, 0)
        ]

    def store(parts, first):
        parts = parts + [jnp.zeros((8, 128), jnp.float32)] * (8 - len(parts))
        rows = packed_sums(parts)
        row = lax.broadcasted_iota(jnp.int32, (8, 128), 0)
        sign = jnp.ones((8, 128), jnp.float32)
        for axis in range(3):
            odd = sum(
                (TRIPLES[first + i][axis] & 1) << i for i in range(8) if first + i < NCOEF
            )
            if odd:
                sign = sign * jnp.where((odd >> row) & 1 == 1, state["flips"][axis], 1.0)
        count = min(8, NCOEF - first)
        leaf_out[first : first + count] = rows[:count]
        flip_ref[first : first + 8] = rows * sign
        sign_ref[first : first + 8] = sign

    def sums_of(orders):
        for p in orders:
            for q in range(ORDER + 1 - p):
                count = ORDER + 1 - p - q

                sums = [None] * count
                for g in range(16):
                    rows = slice(8 * g, 8 * g + 8)
                    term = (a_ref if q == 0 else b_ref)[rows, :]
                    if q < ORDER - p:
                        b_ref[rows, :] = term * v_ref[rows, :]
                    if q == 0 and p < ORDER:
                        a_ref[rows, :] = term * u_ref[rows, :]
                    w = w_ref[rows, :]
                    for r in range(count):
                        sums[r] = term if g == 0 else sums[r] + term
                        if r + 1 < count:
                            term = term * w
                state["sums"] += sums
                while len(state["sums"]) >= 8:
                    store(state["sums"][:8], state["k"])
                    state["sums"] = state["sums"][8:]
                    state["k"] += 8
        if orders[-1] == ORDER:
            store(state["sums"], state["k"])

    def parents():
        high, middle, low = split3(flip_ref[...])
        matrix = table[...]
        shifted = (dot32(matrix, low) + dot32(matrix, middle)) + dot32(matrix, high)
        shifted = shifted * sign_ref[...]
        leaf_row = leaf_final[0:1]
        leaf_col = (
            jnp.broadcast_to(leaf_row.astype(jnp.float32), (CAP, 128)).T.astype(jnp.int32)
        )
        sibling = (
            ((leaf_col >> 3) == (leaf_row >> 3)) & (leaf_col >= 0) & (leaf_row >= 0)
        ).astype(jnp.float32).astype(jnp.bfloat16)
        high, middle, low = split3(shifted)
        total = (dot32(low, sibling) + dot32(middle, sibling)) + dot32(high, sibling)
        parent_out[...] = total[:NCOEF]

    return (
        begin,
        lambda: sums_of((0,)),
        lambda: sums_of((1, 2)),
        lambda: sums_of(tuple(range(3, ORDER + 1))),
        parents,
        turn_x,
        turn_y,
    )


def store_all(final, leaf_final, leaf_in, parent_in, positions, charges, velocities, leaves,
              leaf_out, parent_out, sem):
    pairs = (
        (final.at[0:3], positions),
        (final.at[3], charges),
        (final.at[4:7], velocities),
        (leaf_final.at[0:1], leaves),
        (leaf_in, leaf_out),
        (parent_in, parent_out),
    )
    copies = [pltpu.make_async_copy(*pair, sem.at[k]) for k, pair in enumerate(pairs)]
    for copy in copies:
        copy.start()
    for copy in copies:
        copy.wait()


def per_device(positions, charges, velocities, leaf_ids, live_counts, send_counts):
    vmem = pl.BlockSpec(memory_space=pltpu.VMEM)
    smem = pl.BlockSpec(memory_space=pltpu.SMEM)
    anywhere = pl.BlockSpec(memory_space=pl.ANY)
    f32 = jnp.float32
    copies = len(FRAMES) * len(CHUNKS)
    square = pltpu.VMEM((CAP, 128), f32)
    operands = (
        live_counts,
        send_counts,
        leaf_ids.reshape(1, CAP),
        positions,
        charges,
        velocities,
        shift_table(),
    )
    results = pl.pallas_call(
        exchange,
        name="exchange",
        out_shape=(
            jax.ShapeDtypeStruct((COMPS, CAP, 128), f32),
            jax.ShapeDtypeStruct((8, CAP), jnp.int32),
            jax.ShapeDtypeStruct((NCOEF, CAP), f32),
            jax.ShapeDtypeStruct((NCOEF, CAP), f32),
        ),
        in_specs=[anywhere] * 7,
        out_specs=(vmem,) * 4,
        scratch_shapes=[
            pltpu.SMEM((256,), jnp.int32),
            pltpu.SMEM((8, 256), jnp.int32),
            pltpu.VMEM((1, CAP), jnp.int32),
            pltpu.VMEM((COMPS, LIST_BASE + CAP + 64, 128), f32),
            pltpu.VMEM((COMPS, LIST_BASE + CAP + 64, 128), f32),
            pltpu.VMEM((COMPS, FP_BASE + CAP + 64, 128), f32),
            pltpu.VMEM((COMPS, FR_BASE + 2 * SLAB, 128), f32),
            pltpu.VMEM((COMPS, X_BASE + CAP, 128), f32),
            pltpu.VMEM((2 * len(PHASES), FRAME, 128), f32),
            pltpu.VMEM((3 * len(PHASES), FRAME, 128), f32),
            pltpu.VMEM((ROWS, ROWS), jnp.bfloat16),
        ]
        + [square] * 5
        + [
            pltpu.VMEM((ROWS, 128), f32),
            pltpu.VMEM((ROWS, 128), f32),
            pltpu.SemaphoreType.DMA((4 + COMPS,)),
            pltpu.SemaphoreType.DMA((copies,)),
            pltpu.SemaphoreType.DMA((copies,)),
            pltpu.SemaphoreType.REGULAR,
        ],
        compiler_params=pltpu.CompilerParams(
            collective_id=0, has_side_effects=True, vmem_limit_bytes=VMEM_LIMIT
        ),
    )(*(pltpu.with_memory_space_constraint(operand, pltpu.HBM) for operand in operands))

    outs = pl.pallas_call(
        store_all,
        name="store_all",
        out_shape=(
            jax.ShapeDtypeStruct((3, CAP, 128), f32),
            jax.ShapeDtypeStruct((CAP, 128), f32),
            jax.ShapeDtypeStruct((3, CAP, 128), f32),
            jax.ShapeDtypeStruct((1, CAP), jnp.int32),
            jax.ShapeDtypeStruct((NCOEF, CAP), f32),
            jax.ShapeDtypeStruct((NCOEF, CAP), f32),
        ),
        in_specs=[vmem] * 4,
        out_specs=(anywhere,) * 6,
        scratch_shapes=[pltpu.SemaphoreType.DMA((6,))],
        compiler_params=pltpu.CompilerParams(vmem_limit_bytes=4 * 2**20),
    )(*results)
    moved_positions, moved_charges, moved_velocities, moved_leaves, leaf_part, parent_part = outs
    return (
        moved_positions,
        moved_charges,
        moved_velocities,
        moved_leaves.reshape(CAP),
        leaf_part,
        parent_part,
    )


def solution(mesh):
    names = ("gx", "gy", "gz")
    in_specs = (P(None, names, None), P(names, None), P(None, names, None), P(names), P(), P())
    out_specs = (
        P(None, names, None),
        P(names, None),
        P(None, names, None),
        P(names),
        P(None, names),
        P(None, names),
    )
    return jax.shard_map(
        per_device, mesh=mesh, in_specs=in_specs, out_specs=out_specs, check_vma=False
    )
```
